32 devices in a mesh: slices: 2 (over x), wide: 4 (over y, core), narrow: 4 (over z).
Axes of the slice: x: 2, y: 2, z: 4, core: 2. Of those that a mesh axis runs over, the one named last changes fastest.
Arguments:
- state: float32 [8, 4, 2, 16384], P(('slices', 'wide'), 'narrow'), parts along dimension 0, may hold values from -6 to 6
- gates: float32 [8, 7, 2, 4, 4], replicated, may hold values from -2 to 2
Outputs:
- final_state: float32 [8, 4, 2, 16384], P(('slices', 'wide'), 'narrow'), parts along dimension 0
- marginal: float32 [8, 16384], P(('slices', 'wide'), 'narrow'), parts along dimension 0
The draws below stay inside these ranges and needn't reach their ends.
There are 2 independent parts, one for each index of `slices`. The reference program is written for one: setup_inputs(seed, part) draws one part's arguments, and reference() takes and returns one part's arrays. A program takes and returns all parts, laid end to end along the dimension named above; an argument that names none is the same for every part. Nothing has to cross between parts.
All inputs are finite; a program needn't handle non-finite values.
Results may differ from the reference program's by a relative error of at most 0.0003.
Values sent between devices are 32-bit elements; how exact they have to be, the bound alone decides.
A program may use at most 192 MiB of HBM per device.

```python
import jax
import jax.numpy as jnp
from jax import lax

LAYERS = 8
AMP_DEV = 16384
PAIRS = 7
N_WIDE = 4
N_NARROW = 4


def steps_of(stream_key, dims, shards, low, largest):
    factor_of, own = 1.0, jax.random.fold_in(stream_key, 6)
    for axis_at, blocks in shards:
        heights = jnp.exp(jax.random.uniform(jax.random.fold_in(own, axis_at), (blocks,), jnp.float32, low / len(shards), largest / len(shards)))
        factor_of = factor_of * jnp.repeat(heights, dims[axis_at] // blocks).reshape([-1 if axis == axis_at else 1 for axis in range(len(dims))])
    return factor_of


def noise(stream_key, dims, deviation, most, shards=(), kind=jnp.bfloat16):
    drawn = deviation * jax.random.normal(stream_key, dims, jnp.float32)
    if shards:
        drawn = drawn * steps_of(stream_key, dims, shards, -0.22, 0.18)
    return jnp.clip(drawn, -most, most).astype(kind)


def setup_inputs(seed: int = 0, part: int = 0) -> dict:
    key_list = jax.random.split(jax.random.key(seed), 3)
    part_keys = jax.random.split(jax.random.fold_in(key_list[2], part), 3)
    state = noise(part_keys[0], (N_WIDE, N_NARROW, 2, AMP_DEV), 1.0, 6.0, ((0, 4), (1, 4)), jnp.float32)
    gates = noise(key_list[1], (LAYERS, PAIRS, 2, 4, 4), 8 ** -0.5, 2.0, (), jnp.float32)
    return {"state": state, "gates": gates}


BIT_LETTERS = "abdefghjklmnpqrstuvwxyzABCDEFGHIJKLM"


def apply_gate(psi, gate, low_label, high_label, total_bits):
    letters = BIT_LETTERS[:total_bits]
    low_pos = total_bits - 1 - low_label
    high_pos = total_bits - 1 - high_label
    source = "i" + letters
    target_list = list(letters)
    target_list[high_pos] = "W"
    target_list[low_pos] = "X"
    target = "o" + "".join(target_list)
    real_part = gate[0]
    imag_part = gate[1]
    block = jnp.stack([jnp.stack([real_part, -imag_part]), jnp.stack([imag_part, real_part])])
    block = block.reshape(2, 2, 2, 2, 2, 2)
    gate_form = "oiWX" + letters[high_pos] + letters[low_pos]
    return jnp.einsum(gate_form + "," + source + "->" + target, block, psi, precision=lax.Precision.HIGHEST)


def reference(state, gates):
    high_bits = (N_WIDE * N_NARROW).bit_length() - 1
    local_bits = AMP_DEV.bit_length() - 1
    total_bits = local_bits + high_bits
    psi = jnp.transpose(state, (2, 0, 1, 3)).reshape((2,) + (2,) * total_bits)
    for layer_index in range(LAYERS):
        start = layer_index * high_bits
        for pair_index in range(local_bits // 2):
            low_label = (start + 2 * pair_index) % total_bits
            high_label = (start + 2 * pair_index + 1) % total_bits
            psi = apply_gate(psi, gates[layer_index, pair_index], low_label, high_label, total_bits)
    offset = ((LAYERS - 1) * high_bits) % total_bits
    axes_order = [0] + [1 + total_bits - 1 - ((offset + place) % total_bits) for place in range(total_bits - 1, -1, -1)]
    final = jnp.transpose(psi, axes_order).reshape(2, N_WIDE, N_NARROW, AMP_DEV)
    prob = final[0] * final[0] + final[1] * final[1]
    marginal = jnp.sum(prob, axis=1)
    return jnp.transpose(final, (1, 2, 0, 3)), marginal
```

```python
import functools

import jax
import jax.numpy as jnp
from jax import lax
from jax.experimental import pallas as pl
from jax.experimental.pallas import tpu as pltpu
from jax.sharding import PartitionSpec as P


def kron_chain(members):
    real_part = members[0][0]
    imag_part = members[0][1]
    for member in members[1:]:
        other_real = member[0]
        other_imag = member[1]
        new_real = jnp.kron(real_part, other_real) - jnp.kron(imag_part, other_imag)
        new_imag = jnp.kron(real_part, other_imag) + jnp.kron(imag_part, other_real)
        real_part, imag_part = (new_real, new_imag)
    return (real_part, imag_part)


def rotate(flat, wide_count, narrow_count):
    devices = wide_count * narrow_count
    amplitudes = flat.shape[1]
    rest = amplitudes // devices
    blocks = flat.reshape(2, rest, devices)
    turned = jnp.swapaxes(blocks, 1, 2)
    moved = lax.all_to_all(turned, ("wide", "narrow"), split_axis=1, concat_axis=1, tiled=True)
    return moved.reshape(2, amplitudes)


def apply_layer(flat, layer_gates):
    amplitudes = flat.shape[1]
    pairs = layer_gates.shape[0]
    upper = amplitudes // 256
    low_real, low_imag = kron_chain([layer_gates[index] for index in range(3, -1, -1)])
    high_real, high_imag = kron_chain([layer_gates[index] for index in range(pairs - 1, 3, -1)])
    blocks = flat.reshape(2, upper, 256)
    real_rows = blocks[0]
    imag_rows = blocks[1]
    highest = lax.Precision.HIGHEST
    next_real = jnp.dot(real_rows, low_real.T, precision=highest) - jnp.dot(
        imag_rows, low_imag.T, precision=highest
    )
    next_imag = jnp.dot(real_rows, low_imag.T, precision=highest) + jnp.dot(
        imag_rows, low_real.T, precision=highest
    )
    final_real = jnp.dot(high_real, next_real, precision=highest) - jnp.dot(
        high_imag, next_imag, precision=highest
    )
    final_imag = jnp.dot(high_imag, next_real, precision=highest) + jnp.dot(
        high_real, next_imag, precision=highest
    )
    return jnp.stack([final_real, final_imag]).reshape(2, amplitudes)


MESH = pl.DeviceIdType.MESH
LANES = 128


def complex_mul(left, right):
    return (
        left[0] * right[0] - left[1] * right[1],
        left[0] * right[1] + left[1] * right[0],
    )


def merged_gates(g, plan, order):
    layers, pairs, shift, total_pairs, _, radix = plan
    shape = (2 * radix, LANES)
    lane = lax.broadcasted_iota(jnp.int32, shape, 1)
    down = lax.broadcasted_iota(jnp.int32, shape, 0)
    slots = LANES // (radix * layers)
    layer, row, slot = lane % layers, (lane // layers) % radix, lane // (radix * layers)
    pad = jnp.zeros((radix, LANES - layers), jnp.float32)
    planes = []
    for pair in range(pairs):
        plane = None
        for at in range(radix):
            tile = jnp.concatenate(
                [jnp.concatenate([g[(pair * 2 + c) * radix + at], pad], axis=1) for c in range(2)], axis=0
            )
            tile = jnp.take_along_axis(tile, layer, axis=1, mode="promise_in_bounds")
            plane = tile if plane is None else jnp.where(row == at, tile, plane)
        planes.append(plane)
    unit = jnp.where(down == row, 1.0, 0.0)
    sign = jnp.where(down < radix, -1.0, 1.0)
    found = {}
    for begin in range(0, len(order), slots):
        held = order[begin : begin + slots]
        place = held[0] - shift * layer
        for index, pair in enumerate(held[1:]):
            place = jnp.where(slot == index + 1, pair - shift * layer, place)
        for _ in range(-(-layers * shift // total_pairs)):
            place = jnp.where(place < 0, place + total_pairs, place)
        total = unit
        for pair in range(pairs):
            total = jnp.where(place == pair, planes[pair], total)
        step = 1
        while step < layers:
            source = slot * (radix * layers) + jnp.maximum(layer - step, 0)
            straight, crossed = None, None
            for at in range(radix):
                early = jnp.take_along_axis(total, source + at * layers, axis=1, mode="promise_in_bounds")
                one = total[at : at + 1] * early
                two = total[radix + at : radix + at + 1] * early
                straight = one if straight is None else straight + one
                crossed = two if crossed is None else crossed + two
            total = straight + sign * pltpu.roll(crossed, radix, 0)
            step *= 2
        for index, pair in enumerate(held):
            found[pair] = [
                jnp.broadcast_to(total[:, at : at + 1], shape)
                for at in range(index * radix * layers + layers - 1, (index + 1) * radix * layers, layers)
            ]
    return found


def kron_all(members):
    radix = len(members[0])
    size = radix ** len(members)
    width = max(size, LANES)
    lane = lax.broadcasted_iota(jnp.int32, (2 * radix, width), 1)
    rows = None
    for place, member in enumerate(reversed(members)):
        field = (lane // radix**place) % radix
        columns = [jnp.concatenate([column] * (width // LANES), axis=1) for column in member]
        spread = columns[-1]
        for index in range(radix - 1):
            spread = jnp.where(field == index, columns[index], spread)
        wide = spread[:radix], spread[radix:]
        if rows is None:
            rows = wide
            continue
        pieces = [
            complex_mul(tuple(part[index : index + 1, :] for part in wide), rows)
            for index in range(radix)
        ]
        rows = tuple(jnp.concatenate([piece[c] for piece in pieces], axis=0) for c in range(2))
    return tuple(part[:, :size] for part in rows)


def split(value):
    high = value.astype(jnp.bfloat16)
    return high, (value - high.astype(jnp.float32)).astype(jnp.bfloat16)


def dot(left, right, contract):
    def one(a, b):
        return lax.dot_general(a, b, (((1,), (contract,)), ((), ())), preferred_element_type=jnp.float32)

    return one(left[0], right[0]) + (one(left[0], right[1]) + one(left[1], right[0]))


def greet(semaphore, seat, level):
    pl.semaphore_signal(semaphore, inc=1, device_id={"wide": seat, "narrow": level}, device_id_type=MESH)


def exchange_kernel(plan, x_hbm, g_hbm, recv, lane_hi, lane_lo, row_hi, row_lo, x, g, send,
                    local_sem, send_sem, recv_sem, known):
    layers, pairs, shift, total_pairs, start, radix = plan
    w = lax.axis_index("wide")
    n = lax.axis_index("narrow")
    me = n * radix + w
    count = radix * radix

    barrier = pltpu.get_barrier_semaphore()
    copy_g = pltpu.make_async_copy(g_hbm, g, local_sem.at[0])
    copy_x = pltpu.make_async_copy(x_hbm, x, local_sem.at[1])
    copy_g.start()
    copy_x.start()
    row, core = lax.div(w, 2), lax.rem(w, 2)
    other = 2 * (1 - row)
    seats = [other + core, other + 1 - core, 2 * row + 1 - core, w]
    for level in range(radix):
        @pl.when(level >= n)
        def _():
            for seat in seats[:-1]:
                greet(barrier, seat, level)

            @pl.when(level != n)
            def _():
                greet(barrier, w, level)

    copy_g.wait()
    copy_x.wait()

    order = list(range(start - 1, start + 2)) + list(range(start - 1)) + list(range(start + 2, total_pairs))
    gate = merged_gates(g, plan, order)
    split_gate, low_gate, high_gate = (gate[pair] for pair in range(start - 1, start + 2))

    half = LANES // 2
    group = half // radix
    rows_all = send.shape[1]
    rows_hi = rows_all * radix // (2 * radix - 1)
    tail = rows_hi // radix
    shape = (rows_hi, LANES)
    lane = lax.broadcasted_iota(jnp.int32, shape, 1)
    first = lane < half
    field = (lane // group) % radix
    outer = lane // (2 * group)

    def entry(gate, row, column):
        return tuple(
            jnp.broadcast_to(gate[row][at : at + 1], shape) for at in (column, column + radix)
        )

    def both(gate, one, other):
        return tuple(jnp.where(first, a, b) for a, b in zip(entry(gate, *one), entry(gate, *other)))

    def add(total, term):
        return term if total is None else (total[0] + term[0], total[1] + term[1])

    def roll(value, amount):
        amount %= LANES
        return pltpu.roll(value, amount, 1) if amount else value

    same = [[both(low_gate, (2 * o, 2 * i), (2 * o + 1, 2 * i + 1)) for i in range(2)] for o in range(2)]
    cross = [[both(low_gate, (2 * o, 2 * i + 1), (2 * o + 1, 2 * i)) for i in range(2)] for o in range(2)]
    stage = []
    stride = 4 * radix
    for high in range(radix):
        held = []
        for i in range(2):
            held.append(tuple(x[pl.ds(high * 4 + i * 2 + c, rows_hi, stride=stride), :] for c in range(2)))
        turned = [tuple(roll(v, half) for v in pair) for pair in held]
        result = []
        for o in range(2):
            total = None
            for i in range(2):
                total = add(total, complex_mul(same[o][i], held[i]))
                total = add(total, complex_mul(cross[o][i], turned[i]))
            result.append(total)
        stage.append(result)
    sign = jnp.where(field % 2 == 0, -1.0, 1.0)
    mixers = [[entry(split_gate, take, f) for f in range(radix)] for take in range(radix)]
    mixers = [[(re, im * sign) for re, im in line] for line in mixers]

    def merged(out_high):
        coefs = [entry(high_gate, out_high, high) for high in range(radix)]
        held = []
        for o in range(2):
            total = None
            for high in range(radix):
                total = add(total, complex_mul(coefs[high], stage[high][o]))
            held.append(total)
        return held

    def transposed(held):
        turned = {}
        for o in range(2):
            for c in range(2):
                for d in range(2 * o - 3, 2 * o + 2):
                    turned[o, c, d] = roll(held[o][c], d * group)
        blocks = []
        for f in range(radix):
            pair = []
            for flip in range(2):
                block = None
                for o in range(2):
                    for c in range(2):
                        piece = turned[o, c ^ flip, 2 * o + c - f]
                        block = piece if block is None else jnp.where(field == 2 * o + c, piece, block)
                pair.append(block)
            blocks.append(pair)
        return blocks

    def put(out_high, held, blocks, take):
        real, imag = held[take // 2]
        if take % 2:
            main = jnp.where(first, roll(real, half), imag)
        else:
            main = jnp.where(first, real, roll(imag, half))
        send[out_high * radix + take, :rows_hi] = main
        block = None
        for f in range(radix):
            re, im = mixers[take][f]
            term = re * blocks[f][0] + im * blocks[f][1]
            block = term if block is None else block + term
        spare = (take % 2) * 2 + take // 2
        if spare != radix - 1:
            block = jnp.where(outer == spare, roll(block, 2 * group * (spare + 1)), block)
        moved = [roll(block[rows_hi - tail :], -2 * group * (k + 1)) for k in range(radix - 1)]
        send[out_high * radix + take, rows_hi:] = jnp.where(
            outer[: rows_hi - tail] == radix - 1,
            jnp.concatenate(moved, axis=0),
            block[: rows_hi - tail],
        )

    def post(seat, level):
        pltpu.make_async_remote_copy(
            src_ref=send.at[seat * radix + level],
            dst_ref=recv.at[me],
            send_sem=send_sem,
            recv_sem=recv_sem.at[n],
            device_id={"wide": seat, "narrow": level},
            device_id_type=MESH,
        ).start()

    def lowest(seat):
        @pl.when((n > 0) | (w != seat))
        def _():
            post(seat, 0)

    def below(level, carry):
        for seat in seats:
            post(seat, level)
        return carry

    def above(level, carry):
        pl.semaphore_wait(known.at[level], 1)
        return below(level, carry)

    early = {}
    for out_high in range(2):
        held = merged(out_high)
        early[out_high] = held, transposed(held)
        put(out_high, *early[out_high], 0)

    pl.semaphore_wait(barrier, radix * (n + 1) - 1)
    for seat in range(2):
        lowest(seat)
    for level in range(radix - 1):
        @pl.when(n > level)
        def _():
            greet(known.at[n], w, level)

    for out_high in (2, 3, 0, 1):
        if out_high in early:
            held, blocks = early[out_high]
        else:
            held = merged(out_high)
            blocks = transposed(held)
        for take in range(1 if out_high in early else 0, radix):
            put(out_high, held, blocks, take)

    for seat in range(2, radix):
        lowest(seat)
    lax.fori_loop(1, n, below, 0)

    @pl.when(n > 0)
    def _():
        for seat in seats[:-1]:
            post(seat, n)

    lax.fori_loop(n + 1, radix, above, 0)
    recv[me] = send[w * radix + n]

    low = kron_all([gate[pair] for pair in range(start - 2, -1, -1)])
    block = jnp.concatenate(
        [jnp.concatenate([low[0], low[1]], axis=1), jnp.concatenate([-low[1], low[0]], axis=1)], axis=0
    )
    block = jnp.concatenate([jnp.concatenate([block] * radix, axis=0)] * radix, axis=1)
    down = lax.broadcasted_iota(jnp.int32, (LANES, LANES), 0)
    across = lax.broadcasted_iota(jnp.int32, (LANES, LANES), 1)
    grouped = jnp.where(down // (2 * group) == across // (2 * group), block, 0.0).T
    parts = kron_all([gate[pair] for pair in range(start - 1, -1, -1)])
    plain = jnp.concatenate(
        [jnp.concatenate([parts[0], parts[1]], axis=1), jnp.concatenate([-parts[1], parts[0]], axis=1)],
        axis=0,
    ).T
    for index, item in enumerate((plain, grouped)):
        lane_hi[index], lane_lo[index] = split(item)
    row_members = [gate[pair] for pair in range(total_pairs - 1, start + 1, -1)]
    for index, item in enumerate(kron_all(row_members)):
        for at, held in enumerate(split(item)):
            into = (row_hi, row_lo)[at]
            for source in range(count):
                place = (source % radix) * radix + source // radix
                into[index, place * rows_hi : (place + 1) * rows_hi] = held[source * rows_hi : (source + 1) * rows_hi]

    def settled(group, size):
        return pltpu.make_async_remote_copy(
            src_ref=send.at[pl.ds(0, size)],
            dst_ref=recv.at[pl.ds(0, size)],
            send_sem=send_sem,
            recv_sem=recv_sem.at[group],
            device_id={"wide": w, "narrow": n},
            device_id_type=MESH,
        )

    settled(0, count - 1).wait_send()
    settled(n, radix - 1).wait_recv()
    for step in range(1, radix):
        settled(lax.rem(n + step, radix), radix).wait_recv()


def finish_kernel(radix, recv, lane_hi, lane_lo, row_hi, row_lo, out_hbm, marg_hbm, fin, prob, marg, sems):
    rows_hi = recv.shape[1] * radix // (2 * radix - 1)
    tail = rows_hi // radix
    size = recv.shape[0] * rows_hi
    half = LANES // 2
    group = half // radix
    blocks = size // LANES
    rows = (row_hi[0], row_lo[0]), (row_hi[1], row_lo[1])

    def apply(which, value, keep):
        held = split(value.reshape(size, LANES))
        turned = dot((lane_hi[which], lane_lo[which]), held, 1)
        turned = split(turned[:keep])
        return dot(turned, rows[0], 0), dot(turned, rows[1], 0)

    with_real, with_imag = apply(0, recv[:, :rows_hi], LANES)
    real = with_real[:half] - with_imag[half:]
    imag = with_real[half:] + with_imag[:half]
    for block in range(blocks):
        columns = slice(block * LANES, (block + 1) * LANES)
        fin[pl.ds(block * 2, half, stride=2 * blocks), :] = real[:, columns]
        fin[pl.ds(block * 2 + 1, half, stride=2 * blocks), :] = imag[:, columns]
    out_copy = pltpu.make_async_copy(fin, out_hbm, sems.at[0])
    out_copy.start()
    density = real * real + imag * imag
    for index in range(radix):
        prob[index] = density[index * group : (index + 1) * group]
    packed = recv[:, rows_hi:]
    outer = lax.broadcasted_iota(jnp.int32, (1, tail, LANES), 2) // (2 * group)
    last = None
    for index in range(radix - 1):
        piece = packed[:, index * tail : (index + 1) * tail]
        piece = pltpu.roll(piece, 2 * group * (index + 1), 2)
        last = piece if last is None else jnp.where(outer == index, piece, last)
    wide = jnp.concatenate([packed, last], axis=1)
    with_real, with_imag = apply(1, wide, LANES - 2 * group)
    total = prob[lax.axis_index("narrow")]
    for index in range(radix - 1):
        at = 2 * group * index
        real = with_real[at : at + group] - with_imag[at + group : at + 2 * group]
        imag = with_real[at + group : at + 2 * group] + with_imag[at : at + group]
        term = real * real + imag * imag
        total = total + term
    for block in range(blocks):
        marg[pl.ds(block, group, stride=blocks), :] = total[:, block * LANES : (block + 1) * LANES]
    marg_copy = pltpu.make_async_copy(marg, marg_hbm, sems.at[1])
    marg_copy.start()
    out_copy.wait()
    marg_copy.wait()


def window_plan(wide_count, narrow_count, amplitudes, gates_shape):
    layers, pairs, radix = gates_shape[0], gates_shape[1], gates_shape[-1]
    high_bits = (wide_count * narrow_count).bit_length() - 1
    local_bits = amplitudes.bit_length() - 1
    total_bits = high_bits + local_bits
    if high_bits % 2 or local_bits % 2 or wide_count != radix or narrow_count != radix:
        return None
    if 2 * pairs != local_bits:
        return None
    offset = ((layers - 1) * high_bits) % total_bits
    start = offset // 2 - high_bits // 2
    if layers & (layers - 1) or LANES % (layers * radix) or start < 2 or offset // 2 >= pairs or 2 * radix**start != LANES:
        return None
    rows_hi = radix ** (pairs - offset // 2)
    if rows_hi % 8:
        return None
    for which in range(total_bits // 2):
        if all((which - layer * (high_bits // 2)) % (total_bits // 2) >= pairs for layer in range(layers)):
            return None
    return (layers, pairs, high_bits // 2, total_bits // 2, start, radix), rows_hi


def merged_local(plan, rows_hi, state, gates):
    radix = plan[-1]
    amplitudes = state.shape[-1]
    rows = amplitudes // LANES
    count = radix * radix
    own = amplitudes // radix // LANES
    x = jnp.swapaxes(state.reshape(2, rows, LANES), 0, 1).reshape(2 * rows, LANES)
    g = jnp.transpose(gates, (1, 2, 3, 4, 0)).reshape(-1, radix, gates.shape[0])
    f32, bf16 = jnp.float32, jnp.bfloat16
    size = count * rows_hi
    message = 2 * rows_hi - rows_hi // radix
    shared = (
        pltpu.VMEM((count, message, LANES), f32),
        pltpu.VMEM((2, LANES, LANES), bf16),
        pltpu.VMEM((2, LANES, LANES), bf16),
        pltpu.VMEM((2, size, size), bf16),
        pltpu.VMEM((2, size, size), bf16),
    )
    held = pl.pallas_call(
        functools.partial(exchange_kernel, plan),
        out_shape=shared,
        in_specs=[pl.BlockSpec(memory_space=pltpu.HBM)] * 2,
        out_specs=[pl.BlockSpec(memory_space=pltpu.VMEM)] * len(shared),
        scratch_shapes=[
            pltpu.VMEM(x.shape, f32),
            pltpu.VMEM(g.shape, f32),
            pltpu.VMEM((count, message, LANES), f32),
            pltpu.SemaphoreType.DMA((2,)),
            pltpu.SemaphoreType.DMA,
            pltpu.SemaphoreType.DMA((radix,)),
            pltpu.SemaphoreType.REGULAR((radix,)),
        ],
        compiler_params=pltpu.CompilerParams(
            collective_id=0, has_side_effects=True, vmem_limit_bytes=8 * 2**20
        ),
        name="exchange",
    )(
        pltpu.with_memory_space_constraint(x, pltpu.HBM),
        pltpu.with_memory_space_constraint(g, pltpu.HBM),
    )
    out, marg = pl.pallas_call(
        functools.partial(finish_kernel, radix),
        out_shape=(pltpu.HBM((2 * rows, LANES), f32), pltpu.HBM((own, LANES), f32)),
        in_specs=[pl.BlockSpec(memory_space=pltpu.VMEM)] * len(shared),
        out_specs=[pl.BlockSpec(memory_space=pltpu.HBM)] * 2,
        scratch_shapes=[
            pltpu.VMEM((2 * rows, LANES), f32),
            pltpu.VMEM((radix, LANES // 2 // radix, size), f32),
            pltpu.VMEM((own, LANES), f32),
            pltpu.SemaphoreType.DMA((2,)),
        ],
        compiler_params=pltpu.CompilerParams(vmem_limit_bytes=8 * 2**20),
        name="finish",
    )(*held)
    final = jnp.swapaxes(out.reshape(rows, 2, LANES), 0, 1).reshape(1, 1, 2, amplitudes)
    return final, marg.reshape(1, -1)


def local(state, gates):
    wide_count = lax.axis_size("wide")
    narrow_count = lax.axis_size("narrow")
    amplitudes = state.shape[-1]
    found = window_plan(wide_count, narrow_count, amplitudes, gates.shape)
    if found is not None:
        return merged_local(*found, state, gates)
    flat = state.reshape(2, amplitudes)
    for layer_index in range(gates.shape[0]):
        if layer_index > 0:
            flat = rotate(flat, wide_count, narrow_count)
        flat = apply_layer(flat, gates[layer_index])
    prob = flat[0] * flat[0] + flat[1] * flat[1]
    marginal = lax.psum_scatter(prob, "narrow", scatter_dimension=0, tiled=True)
    return (flat.reshape(1, 1, 2, amplitudes), marginal.reshape(1, -1))


def solution(mesh):
    in_specs = (P(("slices", "wide"), "narrow", None, None), P())
    out_specs = (P(("slices", "wide"), "narrow", None, None), P(("slices", "wide"), "narrow"))
    return jax.shard_map(local, mesh=mesh, in_specs=in_specs, out_specs=out_specs, check_vma=False)
```

```python
import functools

import jax
import jax.numpy as jnp
from jax import lax
from jax.experimental import pallas as pl
from jax.experimental.pallas import tpu as pltpu
from jax.sharding import PartitionSpec as P


def kron_chain(members):
    real_part = members[0][0]
    imag_part = members[0][1]
    for member in members[1:]:
        other_real = member[0]
        other_imag = member[1]
        new_real = jnp.kron(real_part, other_real) - jnp.kron(imag_part, other_imag)
        new_imag = jnp.kron(real_part, other_imag) + jnp.kron(imag_part, other_real)
        real_part, imag_part = (new_real, new_imag)
    return (real_part, imag_part)


def rotate(flat, wide_count, narrow_count):
    devices = wide_count * narrow_count
    amplitudes = flat.shape[1]
    rest = amplitudes // devices
    blocks = flat.reshape(2, rest, devices)
    turned = jnp.swapaxes(blocks, 1, 2)
    moved = lax.all_to_all(turned, ("wide", "narrow"), split_axis=1, concat_axis=1, tiled=True)
    return moved.reshape(2, amplitudes)


def apply_layer(flat, layer_gates):
    amplitudes = flat.shape[1]
    pairs = layer_gates.shape[0]
    upper = amplitudes // 256
    low_real, low_imag = kron_chain([layer_gates[index] for index in range(3, -1, -1)])
    high_real, high_imag = kron_chain([layer_gates[index] for index in range(pairs - 1, 3, -1)])
    blocks = flat.reshape(2, upper, 256)
    real_rows = blocks[0]
    imag_rows = blocks[1]
    highest = lax.Precision.HIGHEST
    next_real = jnp.dot(real_rows, low_real.T, precision=highest) - jnp.dot(
        imag_rows, low_imag.T, precision=highest
    )
    next_imag = jnp.dot(real_rows, low_imag.T, precision=highest) + jnp.dot(
        imag_rows, low_real.T, precision=highest
    )
    final_real = jnp.dot(high_real, next_real, precision=highest) - jnp.dot(
        high_imag, next_imag, precision=highest
    )
    final_imag = jnp.dot(high_imag, next_real, precision=highest) + jnp.dot(
        high_real, next_imag, precision=highest
    )
    return jnp.stack([final_real, final_imag]).reshape(2, amplitudes)


MESH = pl.DeviceIdType.MESH
LANES = 128


def complex_mul(left, right):
    return (
        left[0] * right[0] - left[1] * right[1],
        left[0] * right[1] + left[1] * right[0],
    )


def take_lanes(value, source):
    return jnp.take_along_axis(value, source, axis=1, mode="promise_in_bounds")


def gate_tools(g, plan):
    layers, pairs, shift, total_pairs, _, radix = plan
    shape = (2 * radix, LANES)
    lane = lax.broadcasted_iota(jnp.int32, shape, 1)
    down = lax.broadcasted_iota(jnp.int32, shape, 0)
    width = radix * layers
    layer, row, slot = lane % layers, (lane // layers) % radix, lane // width
    pad = jnp.zeros((radix, LANES - layers), jnp.float32)
    tiles, planes = [], []
    for pair in range(pairs):
        tiles.append([])
        plane = None
        for at in range(radix):
            tile = jnp.concatenate(
                [jnp.concatenate([g[(pair * 2 + c) * radix + at], pad], axis=1) for c in range(2)], axis=0
            )
            tiles[-1].append(tile)
            tile = take_lanes(tile, layer)
            plane = tile if plane is None else jnp.where(row == at, tile, plane)
        planes.append(plane)
    sign = jnp.where(down < radix, -1.0, 1.0)

    def merge(held, direct=False):
        place = held[0] - shift * layer
        for index, pair in enumerate(held[1:]):
            place = jnp.where(slot == index + 1, pair - shift * layer, place)
        for _ in range(-(-layers * shift // total_pairs)):
            place = jnp.where(place < 0, place + total_pairs, place)
        total = jnp.where(down == row, 1.0, 0.0)
        for pair in range(pairs):
            total = jnp.where(place == pair, planes[pair], total)
        step = 1
        while step < layers:
            before = jnp.maximum(layer - step, 0)
            straight, crossed = None, None
            for at in range(radix):
                if direct and step == 1:
                    early = jnp.where(down == at, 1.0, 0.0)
                    previous = jnp.where(place + shift < total_pairs, place + shift, place + shift - total_pairs)
                    for pair in range(pairs):
                        early = jnp.where(previous == pair, take_lanes(tiles[pair][at], before), early)
                else:
                    early = take_lanes(total, slot * width + at * layers + before)
                one_part = total[at : at + 1] * early
                two_part = total[radix + at : radix + at + 1] * early
                straight = one_part if straight is None else straight + one_part
                crossed = two_part if crossed is None else crossed + two_part
            total = straight + sign * pltpu.roll(crossed, radix, 0)
            step *= 2
        return {
            pair: [
                take_lanes(total, jnp.full(shape, index * width + (at + 1) * layers - 1, jnp.int32))
                for at in range(radix)
            ]
            for index, pair in enumerate(held)
        }

    return merge


def kron_all(members):
    radix = len(members[0])
    size = radix ** len(members)
    width = max(size, LANES)
    lane = lax.broadcasted_iota(jnp.int32, (2 * radix, width), 1)
    rows = None
    for place, member in enumerate(reversed(members)):
        field = (lane // radix**place) % radix
        columns = [jnp.concatenate([column] * (width // LANES), axis=1) for column in member]
        spread = columns[-1]
        for index in range(radix - 1):
            spread = jnp.where(field == index, columns[index], spread)
        wide = spread[:radix], spread[radix:]
        if rows is None:
            rows = wide
            continue
        pieces = [
            complex_mul(tuple(part[index : index + 1, :] for part in wide), rows)
            for index in range(radix)
        ]
        rows = tuple(jnp.concatenate([piece[c] for piece in pieces], axis=0) for c in range(2))
    return tuple(part[:, :size] for part in rows)


def split(value):
    high = value.astype(jnp.bfloat16)
    return high, (value - high.astype(jnp.float32)).astype(jnp.bfloat16)


def dot(left, right, contract):
    def one(a, b):
        return lax.dot_general(a, b, (((1,), (contract,)), ((), ())), preferred_element_type=jnp.float32)

    return one(left[0], right[0]) + (one(left[0], right[1]) + one(left[1], right[0]))


def greet(semaphore, seat, level):
    pl.semaphore_signal(semaphore, inc=1, device_id={"wide": seat, "narrow": level}, device_id_type=MESH)


def exchange_kernel(plan, x_hbm, g_hbm, recv, lane_hi, lane_lo, row_hi, row_lo, x, g, send,
                    local_sem, send_sem, recv_sem, known):
    layers, pairs, shift, total_pairs, start, radix = plan
    w = lax.axis_index("wide")
    n = lax.axis_index("narrow")
    me = n * radix + w
    count = radix * radix

    barrier = pltpu.get_barrier_semaphore()
    copy_g = pltpu.make_async_copy(g_hbm, g, local_sem.at[0])
    copy_x = pltpu.make_async_copy(x_hbm, x, local_sem.at[1])
    copy_g.start()
    copy_x.start()
    row, core = lax.div(w, 2), lax.rem(w, 2)
    other = 2 * (1 - row)
    seats = [other + core, other + 1 - core, 2 * row + 1 - core, w]
    for level in range(1, radix):
        @pl.when(level > n)
        def _():
            for seat in range(radix):
                greet(barrier, seat, level)

    for seat in range(1, radix):
        @pl.when(seat > w)
        def _():
            greet(barrier, seat, n)

    @pl.when(me > 0)
    def _():
        pl.semaphore_wait(barrier, me)

    for level in range(radix - 1):
        @pl.when(level < n)
        def _():
            for seat in range(radix):
                greet(known.at[n], seat, level)

    for seat in range(radix - 1):
        @pl.when(seat < w)
        def _():
            greet(known.at[n], seat, n)

    copy_g.wait()
    copy_x.wait()

    merge = gate_tools(g, plan)
    order = list(range(start - 1, start + 2)) + list(range(start - 1)) + list(range(start + 2, total_pairs))
    slots = LANES // (radix * layers)
    gate = merge(order[:slots], True)
    split_gate, low_gate, high_gate = (gate[pair] for pair in range(start - 1, start + 2))

    half = LANES // 2
    group = half // radix
    rows_all = send.shape[1]
    rows_hi = rows_all * radix // (2 * radix - 1)
    tail = rows_hi // radix
    shape = (rows_hi, LANES)
    lane = lax.broadcasted_iota(jnp.int32, shape, 1)
    first = lane < half
    field = (lane // group) % radix
    outer = lane // (2 * group)

    def entry(gate, row, column):
        return tuple(
            jnp.broadcast_to(gate[row][at : at + 1], shape) for at in (column, column + radix)
        )

    def both(gate, one, other):
        return tuple(jnp.where(first, a, b) for a, b in zip(entry(gate, *one), entry(gate, *other)))

    def add(total, term):
        return term if total is None else (total[0] + term[0], total[1] + term[1])

    def roll(value, amount):
        amount %= LANES
        return pltpu.roll(value, amount, 1) if amount else value

    same = [[both(low_gate, (2 * o, 2 * i), (2 * o + 1, 2 * i + 1)) for i in range(2)] for o in range(2)]
    cross = [[both(low_gate, (2 * o, 2 * i + 1), (2 * o + 1, 2 * i)) for i in range(2)] for o in range(2)]
    stage = []
    stride = 4 * radix
    for high in range(radix):
        held = []
        for i in range(2):
            held.append(tuple(x[pl.ds(high * 4 + i * 2 + c, rows_hi, stride=stride), :] for c in range(2)))
        turned = [tuple(roll(v, half) for v in pair) for pair in held]
        result = []
        for o in range(2):
            total = None
            for i in range(2):
                total = add(total, complex_mul(same[o][i], held[i]))
                total = add(total, complex_mul(cross[o][i], turned[i]))
            result.append(total)
        stage.append(result)
    sign = jnp.where(field % 2 == 0, -1.0, 1.0)
    mixers = [[entry(split_gate, take, f) for f in range(radix)] for take in range(radix)]
    mixers = [[(re, im * sign) for re, im in line] for line in mixers]

    def merged(out_high):
        coefs = [entry(high_gate, out_high, high) for high in range(radix)]
        held = []
        for o in range(2):
            total = None
            for high in range(radix):
                total = add(total, complex_mul(coefs[high], stage[high][o]))
            held.append(total)
        return held

    def transposed(held):
        turned = {}
        for o in range(2):
            for c in range(2):
                for d in range(2 * o - 3, 2 * o + 2):
                    turned[o, c, d] = roll(held[o][c], d * group)
        blocks = []
        for f in range(radix):
            pair = []
            for flip in range(2):
                block = None
                for o in range(2):
                    for c in range(2):
                        piece = turned[o, c ^ flip, 2 * o + c - f]
                        block = piece if block is None else jnp.where(field == 2 * o + c, piece, block)
                pair.append(block)
            blocks.append(pair)
        return blocks

    def put_main(out_high, held, take):
        real, imag = held[take // 2]
        if take % 2:
            main = jnp.where(first, roll(real, half), imag)
        else:
            main = jnp.where(first, real, roll(imag, half))
        send[out_high * radix + take, :rows_hi] = main

    def put_extra(out_high, blocks, take):
        block = None
        for f in range(radix):
            re, im = mixers[take][f]
            term = re * blocks[f][0] + im * blocks[f][1]
            block = term if block is None else block + term
        own = (take % 2) * 2 + take // 2
        moved = [roll(block[rows_hi - tail :], 2 * group * (own - k)) for k in range(radix) if k != own]
        send[out_high * radix + take, rows_hi:] = jnp.where(
            outer[: rows_hi - tail] == own, jnp.concatenate(moved, axis=0), block[: rows_hi - tail]
        )

    def post(seat, level, rows):
        pltpu.make_async_remote_copy(
            src_ref=send.at[seat * radix + level, rows],
            dst_ref=recv.at[me, rows],
            send_sem=send_sem,
            recv_sem=recv_sem.at[n],
            device_id={"wide": seat, "narrow": level},
            device_id_type=MESH,
        ).start()

    def lowest(first_seat, rows):
        last_seat = first_seat + 1
        alone = (n == 0) & (lax.div(w, 2) == first_seat // 2)
        other_seat = first_seat + last_seat - w

        def body(seat, carry):
            post(seat, 0, rows)
            return carry

        lax.fori_loop(
            jnp.where(alone, other_seat, first_seat), jnp.where(alone, other_seat, last_seat) + 1, body, 0
        )

    whole = pl.ds(0, rows_all)

    def below(level, carry):
        for seat in seats:
            post(seat, level, whole)
        return carry

    def above(level, carry):
        pl.semaphore_wait(known.at[level], radix)
        return below(level, carry)

    early, opened = {}, {}
    for out_high in range(2):
        early[out_high] = merged(out_high)
        put_main(out_high, early[out_high], 0)
        opened[out_high] = transposed(early[out_high])
        put_extra(out_high, opened[out_high], 0)

    peers = radix - 1 - w

    @pl.when((n == 0) & (peers > 0))
    def _():
        pl.semaphore_wait(known.at[n], peers)

    lowest(0, whole)

    for out_high in (2, 3, 0, 1):
        if out_high in early:
            held, blocks = early[out_high], opened[out_high]
        else:
            held = merged(out_high)
            blocks = transposed(held)
        for take in range(1 if out_high in early else 0, radix):
            put_main(out_high, held, take)
            put_extra(out_high, blocks, take)

    lowest(2, whole)
    lax.fori_loop(1, n, below, 0)

    @pl.when(n > 0)
    def _():
        @pl.when(peers > 0)
        def _():
            pl.semaphore_wait(known.at[n], peers)

        for seat in seats[:-1]:
            post(seat, n, whole)

    lax.fori_loop(n + 1, radix, above, 0)
    recv[me] = send[w * radix + n]

    for begin in range(slots, total_pairs, slots):
        gate.update(merge(order[begin : begin + slots]))
    low = kron_all([gate[pair] for pair in range(start - 2, -1, -1)])
    block = jnp.concatenate(
        [jnp.concatenate([low[0], low[1]], axis=1), jnp.concatenate([-low[1], low[0]], axis=1)], axis=0
    )
    block = jnp.concatenate([jnp.concatenate([block] * radix, axis=0)] * radix, axis=1)
    down = lax.broadcasted_iota(jnp.int32, (LANES, LANES), 0)
    across = lax.broadcasted_iota(jnp.int32, (LANES, LANES), 1)
    grouped = jnp.where(down // (2 * group) == across // (2 * group), block, 0.0).T
    parts = kron_all([gate[pair] for pair in range(start - 1, -1, -1)])
    plain = jnp.concatenate(
        [jnp.concatenate([parts[0], parts[1]], axis=1), jnp.concatenate([-parts[1], parts[0]], axis=1)],
        axis=0,
    ).T
    for index, item in enumerate((plain, grouped)):
        lane_hi[index], lane_lo[index] = split(item)
    row_members = [gate[pair] for pair in range(total_pairs - 1, start + 1, -1)]
    for index, item in enumerate(kron_all(row_members)):
        for at, held in enumerate(split(item)):
            into = (row_hi, row_lo)[at]
            for source in range(count):
                place = (source % radix) * radix + source // radix
                into[index, place * rows_hi : (place + 1) * rows_hi] = held[source * rows_hi : (source + 1) * rows_hi]

    def settled(group, size):
        return pltpu.make_async_remote_copy(
            src_ref=send.at[pl.ds(0, size)],
            dst_ref=recv.at[pl.ds(0, size)],
            send_sem=send_sem,
            recv_sem=recv_sem.at[group],
            device_id={"wide": w, "narrow": n},
            device_id_type=MESH,
        )

    settled(0, count - 1).wait_send()
    settled(n, radix - 1).wait_recv()
    for step in range(1, radix):
        settled(lax.rem(n + step, radix), radix).wait_recv()


def finish_kernel(radix, recv, lane_hi, lane_lo, row_hi, row_lo, out_hbm, marg_hbm, fin, prob, marg, sems):
    rows_hi = recv.shape[1] * radix // (2 * radix - 1)
    tail = rows_hi // radix
    size = recv.shape[0] * rows_hi
    half = LANES // 2
    group = half // radix
    blocks = size // LANES
    rows = (row_hi[0], row_lo[0]), (row_hi[1], row_lo[1])

    def apply(which, value, keep):
        held = split(value.reshape(size, LANES))
        turned = dot((lane_hi[which], lane_lo[which]), held, 1)
        turned = split(turned[:keep])
        return dot(turned, rows[0], 0), dot(turned, rows[1], 0)

    with_real, with_imag = apply(0, recv[:, :rows_hi], LANES)
    real = with_real[:half] - with_imag[half:]
    imag = with_real[half:] + with_imag[:half]
    for block in range(blocks):
        columns = slice(block * LANES, (block + 1) * LANES)
        fin[pl.ds(block * 2, half, stride=2 * blocks), :] = real[:, columns]
        fin[pl.ds(block * 2 + 1, half, stride=2 * blocks), :] = imag[:, columns]
    out_copy = pltpu.make_async_copy(fin, out_hbm, sems.at[0])
    out_copy.start()
    density = real * real + imag * imag
    for index in range(radix):
        prob[index] = density[index * group : (index + 1) * group]
    packed = recv[:, rows_hi:]
    outer = lax.broadcasted_iota(jnp.int32, (1, tail, LANES), 2) // (2 * group)
    n = lax.axis_index("narrow")
    own = (n % 2) * 2 + n // 2
    last = packed[:, :tail]
    for index in range(radix - 1):
        kept = index + jnp.where(own <= index, 1, 0)
        piece = packed[:, index * tail : (index + 1) * tail]
        piece = pltpu.roll(piece, lax.rem(2 * group * (kept - own) + LANES, LANES), 2)
        last = jnp.where(outer == kept, piece, last)
    wide = jnp.concatenate([packed, last], axis=1)
    with_real, with_imag = apply(1, wide, LANES)
    total = prob[n]
    for index in range(radix):
        at = 2 * group * index
        real = with_real[at : at + group] - with_imag[at + group : at + 2 * group]
        imag = with_real[at + group : at + 2 * group] + with_imag[at : at + group]
        total = total + jnp.where(own == index, 0.0, real * real + imag * imag)
    for block in range(blocks):
        marg[pl.ds(block, group, stride=blocks), :] = total[:, block * LANES : (block + 1) * LANES]
    marg_copy = pltpu.make_async_copy(marg, marg_hbm, sems.at[1])
    marg_copy.start()
    out_copy.wait()
    marg_copy.wait()


def window_plan(wide_count, narrow_count, amplitudes, gates_shape):
    layers, pairs, radix = gates_shape[0], gates_shape[1], gates_shape[-1]
    high_bits = (wide_count * narrow_count).bit_length() - 1
    local_bits = amplitudes.bit_length() - 1
    total_bits = high_bits + local_bits
    if high_bits % 2 or local_bits % 2 or wide_count != radix or narrow_count != radix:
        return None
    if 2 * pairs != local_bits:
        return None
    offset = ((layers - 1) * high_bits) % total_bits
    start = offset // 2 - high_bits // 2
    if layers & (layers - 1) or LANES % (layers * radix) or start < 2 or LANES < 3 * layers * radix or offset // 2 >= pairs or 2 * radix**start != LANES:
        return None
    rows_hi = radix ** (pairs - offset // 2)
    if rows_hi % 8:
        return None
    for which in range(total_bits // 2):
        if all((which - layer * (high_bits // 2)) % (total_bits // 2) >= pairs for layer in range(layers)):
            return None
    return (layers, pairs, high_bits // 2, total_bits // 2, start, radix), rows_hi


def merged_local(plan, rows_hi, state, gates):
    radix = plan[-1]
    amplitudes = state.shape[-1]
    rows = amplitudes // LANES
    count = radix * radix
    own = amplitudes // radix // LANES
    x = jnp.swapaxes(state.reshape(2, rows, LANES), 0, 1).reshape(2 * rows, LANES)
    g = jnp.transpose(gates, (1, 2, 3, 4, 0)).reshape(-1, radix, gates.shape[0])
    f32, bf16 = jnp.float32, jnp.bfloat16
    size = count * rows_hi
    message = 2 * rows_hi - rows_hi // radix
    shared = (
        pltpu.VMEM((count, message, LANES), f32),
        pltpu.VMEM((2, LANES, LANES), bf16),
        pltpu.VMEM((2, LANES, LANES), bf16),
        pltpu.VMEM((2, size, size), bf16),
        pltpu.VMEM((2, size, size), bf16),
    )
    held = pl.pallas_call(
        functools.partial(exchange_kernel, plan),
        out_shape=shared,
        in_specs=[pl.BlockSpec(memory_space=pltpu.HBM)] * 2,
        out_specs=[pl.BlockSpec(memory_space=pltpu.VMEM)] * len(shared),
        scratch_shapes=[
            pltpu.VMEM(x.shape, f32),
            pltpu.VMEM(g.shape, f32),
            pltpu.VMEM((count, message, LANES), f32),
            pltpu.SemaphoreType.DMA((2,)),
            pltpu.SemaphoreType.DMA,
            pltpu.SemaphoreType.DMA((radix,)),
            pltpu.SemaphoreType.REGULAR((radix,)),
        ],
        compiler_params=pltpu.CompilerParams(
            collective_id=0, has_side_effects=True, vmem_limit_bytes=8 * 2**20
        ),
        name="exchange",
    )(
        pltpu.with_memory_space_constraint(x, pltpu.HBM),
        pltpu.with_memory_space_constraint(g, pltpu.HBM),
    )
    out, marg = pl.pallas_call(
        functools.partial(finish_kernel, radix),
        out_shape=(pltpu.HBM((2 * rows, LANES), f32), pltpu.HBM((own, LANES), f32)),
        in_specs=[pl.BlockSpec(memory_space=pltpu.VMEM)] * len(shared),
        out_specs=[pl.BlockSpec(memory_space=pltpu.HBM)] * 2,
        scratch_shapes=[
            pltpu.VMEM((2 * rows, LANES), f32),
            pltpu.VMEM((radix, LANES // 2 // radix, size), f32),
            pltpu.VMEM((own, LANES), f32),
            pltpu.SemaphoreType.DMA((2,)),
        ],
        compiler_params=pltpu.CompilerParams(vmem_limit_bytes=8 * 2**20),
        name="finish",
    )(*held)
    final = jnp.swapaxes(out.reshape(rows, 2, LANES), 0, 1).reshape(1, 1, 2, amplitudes)
    return final, marg.reshape(1, -1)


def local(state, gates):
    wide_count = lax.axis_size("wide")
    narrow_count = lax.axis_size("narrow")
    amplitudes = state.shape[-1]
    found = window_plan(wide_count, narrow_count, amplitudes, gates.shape)
    if found is not None:
        return merged_local(*found, state, gates)
    flat = state.reshape(2, amplitudes)
    for layer_index in range(gates.shape[0]):
        if layer_index > 0:
            flat = rotate(flat, wide_count, narrow_count)
        flat = apply_layer(flat, gates[layer_index])
    prob = flat[0] * flat[0] + flat[1] * flat[1]
    marginal = lax.psum_scatter(prob, "narrow", scatter_dimension=0, tiled=True)
    return (flat.reshape(1, 1, 2, amplitudes), marginal.reshape(1, -1))


def solution(mesh):
    in_specs = (P(("slices", "wide"), "narrow", None, None), P())
    out_specs = (P(("slices", "wide"), "narrow", None, None), P(("slices", "wide"), "narrow"))
    return jax.shard_map(local, mesh=mesh, in_specs=in_specs, out_specs=out_specs, check_vma=False)
```

```python
import functools

import jax
import jax.numpy as jnp
from jax import lax
from jax.experimental import pallas as pl
from jax.experimental.pallas import tpu as pltpu
from jax.sharding import PartitionSpec as P


def kron_chain(members):
    real_part = members[0][0]
    imag_part = members[0][1]
    for member in members[1:]:
        other_real = member[0]
        other_imag = member[1]
        new_real = jnp.kron(real_part, other_real) - jnp.kron(imag_part, other_imag)
        new_imag = jnp.kron(real_part, other_imag) + jnp.kron(imag_part, other_real)
        real_part, imag_part = (new_real, new_imag)
    return (real_part, imag_part)


def rotate(flat, wide_count, narrow_count):
    devices = wide_count * narrow_count
    amplitudes = flat.shape[1]
    rest = amplitudes // devices
    blocks = flat.reshape(2, rest, devices)
    turned = jnp.swapaxes(blocks, 1, 2)
    moved = lax.all_to_all(turned, ("wide", "narrow"), split_axis=1, concat_axis=1, tiled=True)
    return moved.reshape(2, amplitudes)


def apply_layer(flat, layer_gates):
    amplitudes = flat.shape[1]
    pairs = layer_gates.shape[0]
    upper = amplitudes // 256
    low_real, low_imag = kron_chain([layer_gates[index] for index in range(3, -1, -1)])
    high_real, high_imag = kron_chain([layer_gates[index] for index in range(pairs - 1, 3, -1)])
    blocks = flat.reshape(2, upper, 256)
    real_rows = blocks[0]
    imag_rows = blocks[1]
    highest = lax.Precision.HIGHEST
    next_real = jnp.dot(real_rows, low_real.T, precision=highest) - jnp.dot(
        imag_rows, low_imag.T, precision=highest
    )
    next_imag = jnp.dot(real_rows, low_imag.T, precision=highest) + jnp.dot(
        imag_rows, low_real.T, precision=highest
    )
    final_real = jnp.dot(high_real, next_real, precision=highest) - jnp.dot(
        high_imag, next_imag, precision=highest
    )
    final_imag = jnp.dot(high_imag, next_real, precision=highest) + jnp.dot(
        high_real, next_imag, precision=highest
    )
    return jnp.stack([final_real, final_imag]).reshape(2, amplitudes)


MESH = pl.DeviceIdType.MESH
LANES = 128


def complex_mul(left, right):
    return (
        left[0] * right[0] - left[1] * right[1],
        left[0] * right[1] + left[1] * right[0],
    )


def take_lanes(value, source):
    return jnp.take_along_axis(value, source, axis=1, mode="promise_in_bounds")


def gate_tools(g, plan):
    layers, pairs, shift, total_pairs, _, radix = plan
    shape = (2 * radix, LANES)
    lane = lax.broadcasted_iota(jnp.int32, shape, 1)
    down = lax.broadcasted_iota(jnp.int32, shape, 0)
    width = radix * layers
    layer, row, slot = lane % layers, (lane // layers) % radix, lane // width
    pad = jnp.zeros((radix, LANES - layers), jnp.float32)
    tiles, planes = [], []
    for pair in range(pairs):
        tiles.append([])
        plane = None
        for at in range(radix):
            tile = jnp.concatenate(
                [jnp.concatenate([g[(pair * 2 + c) * radix + at], pad], axis=1) for c in range(2)], axis=0
            )
            tiles[-1].append(tile)
            tile = take_lanes(tile, layer)
            plane = tile if plane is None else jnp.where(row == at, tile, plane)
        planes.append(plane)
    sign = jnp.where(down < radix, -1.0, 1.0)

    def merge(held, direct=False):
        place = held[0] - shift * layer
        for index, pair in enumerate(held[1:]):
            place = jnp.where(slot == index + 1, pair - shift * layer, place)
        for _ in range(-(-layers * shift // total_pairs)):
            place = jnp.where(place < 0, place + total_pairs, place)
        total = jnp.where(down == row, 1.0, 0.0)
        for pair in range(pairs):
            total = jnp.where(place == pair, planes[pair], total)
        step = 1
        while step < layers:
            before = jnp.maximum(layer - step, 0)
            straight, crossed = None, None
            for at in range(radix):
                if direct and step == 1:
                    early = jnp.where(down == at, 1.0, 0.0)
                    previous = jnp.where(place + shift < total_pairs, place + shift, place + shift - total_pairs)
                    for pair in range(pairs):
                        early = jnp.where(previous == pair, take_lanes(tiles[pair][at], before), early)
                else:
                    early = take_lanes(total, slot * width + at * layers + before)
                one_part = total[at : at + 1] * early
                two_part = total[radix + at : radix + at + 1] * early
                straight = one_part if straight is None else straight + one_part
                crossed = two_part if crossed is None else crossed + two_part
            total = straight + sign * pltpu.roll(crossed, radix, 0)
            step *= 2
        return {
            pair: [
                take_lanes(total, jnp.full(shape, index * width + (at + 1) * layers - 1, jnp.int32))
                for at in range(radix)
            ]
            for index, pair in enumerate(held)
        }

    return merge


def kron_all(members):
    radix = len(members[0])
    size = radix ** len(members)
    width = max(size, LANES)
    lane = lax.broadcasted_iota(jnp.int32, (2 * radix, width), 1)
    rows = None
    for place, member in enumerate(reversed(members)):
        field = (lane // radix**place) % radix
        columns = [jnp.concatenate([column] * (width // LANES), axis=1) for column in member]
        spread = columns[-1]
        for index in range(radix - 1):
            spread = jnp.where(field == index, columns[index], spread)
        wide = spread[:radix], spread[radix:]
        if rows is None:
            rows = wide
            continue
        pieces = [
            complex_mul(tuple(part[index : index + 1, :] for part in wide), rows)
            for index in range(radix)
        ]
        rows = tuple(jnp.concatenate([piece[c] for piece in pieces], axis=0) for c in range(2))
    return tuple(part[:, :size] for part in rows)


def split(value):
    high = value.astype(jnp.bfloat16)
    return high, (value - high.astype(jnp.float32)).astype(jnp.bfloat16)


def dot(left, right, contract):
    def one(a, b):
        return lax.dot_general(a, b, (((1,), (contract,)), ((), ())), preferred_element_type=jnp.float32)

    return one(left[0], right[0]) + (one(left[0], right[1]) + one(left[1], right[0]))


def greet(semaphore, seat, level):
    pl.semaphore_signal(semaphore, inc=1, device_id={"wide": seat, "narrow": level}, device_id_type=MESH)


def exchange_kernel(plan, x_hbm, g_hbm, recv, lane_hi, lane_lo, row_hi, row_lo, x, g, send,
                    local_sem, send_sem, recv_sem, known):
    layers, pairs, shift, total_pairs, start, radix = plan
    w = lax.axis_index("wide")
    n = lax.axis_index("narrow")
    me = n * radix + w
    count = radix * radix

    barrier = pltpu.get_barrier_semaphore()
    copy_g = pltpu.make_async_copy(g_hbm, g, local_sem.at[0])
    copy_x = pltpu.make_async_copy(x_hbm, x, local_sem.at[1])
    copy_g.start()
    copy_x.start()
    row, core = lax.div(w, 2), lax.rem(w, 2)
    other = 2 * (1 - row)
    seats = [other + core, other + 1 - core, 2 * row + 1 - core, w]
    for level in range(1, radix):
        @pl.when(level > n)
        def _():
            for seat in range(radix):
                greet(barrier, seat, level)

    for seat in range(1, radix):
        @pl.when(seat > w)
        def _():
            greet(barrier, seat, n)

    @pl.when(me > 0)
    def _():
        pl.semaphore_wait(barrier, me)

    for level in range(radix - 1):
        @pl.when(level < n)
        def _():
            for seat in range(radix):
                greet(known.at[n], seat, level)

    for seat in range(radix - 1):
        @pl.when(seat < w)
        def _():
            greet(known.at[n], seat, n)

    copy_g.wait()
    copy_x.wait()

    merge = gate_tools(g, plan)
    order = list(range(start - 1, start + 2)) + list(range(start - 1)) + list(range(start + 2, total_pairs))
    slots = LANES // (radix * layers)
    gate = merge(order[:slots], True)
    split_gate, low_gate, high_gate = (gate[pair] for pair in range(start - 1, start + 2))

    half = LANES // 2
    group = half // radix
    rows_all = send.shape[1]
    rows_hi = rows_all * radix // (2 * radix - 1)
    tail = rows_hi // radix
    shape = (rows_hi, LANES)
    lane = lax.broadcasted_iota(jnp.int32, shape, 1)
    first = lane < half
    field = (lane // group) % radix
    outer = lane // (2 * group)

    def entry(gate, row, column):
        return tuple(
            jnp.broadcast_to(gate[row][at : at + 1], shape) for at in (column, column + radix)
        )

    def both(gate, one, other):
        return tuple(jnp.where(first, a, b) for a, b in zip(entry(gate, *one), entry(gate, *other)))

    def add(total, term):
        return term if total is None else (total[0] + term[0], total[1] + term[1])

    def roll(value, amount):
        amount %= LANES
        return pltpu.roll(value, amount, 1) if amount else value

    same = [[both(low_gate, (2 * o, 2 * i), (2 * o + 1, 2 * i + 1)) for i in range(2)] for o in range(2)]
    cross = [[both(low_gate, (2 * o, 2 * i + 1), (2 * o + 1, 2 * i)) for i in range(2)] for o in range(2)]
    stage = []
    stride = 4 * radix
    for high in range(radix):
        held = []
        for i in range(2):
            held.append(tuple(x[pl.ds(high * 4 + i * 2 + c, rows_hi, stride=stride), :] for c in range(2)))
        turned = [tuple(roll(v, half) for v in pair) for pair in held]
        result = []
        for o in range(2):
            total = None
            for i in range(2):
                total = add(total, complex_mul(same[o][i], held[i]))
                total = add(total, complex_mul(cross[o][i], turned[i]))
            result.append(total)
        stage.append(result)
    sign = jnp.where(field % 2 == 0, -1.0, 1.0)
    mixers = [[entry(split_gate, take, f) for f in range(radix)] for take in range(radix)]
    mixers = [[(re, im * sign) for re, im in line] for line in mixers]

    def merged(out_high):
        coefs = [entry(high_gate, out_high, high) for high in range(radix)]
        held = []
        for o in range(2):
            total = None
            for high in range(radix):
                total = add(total, complex_mul(coefs[high], stage[high][o]))
            held.append(total)
        return held

    def transposed(held):
        turned = {}
        for o in range(2):
            for c in range(2):
                for d in range(2 * o - 3, 2 * o + 2):
                    turned[o, c, d] = roll(held[o][c], d * group)
        blocks = []
        for f in range(radix):
            pair = []
            for flip in range(2):
                block = None
                for o in range(2):
                    for c in range(2):
                        piece = turned[o, c ^ flip, 2 * o + c - f]
                        block = piece if block is None else jnp.where(field == 2 * o + c, piece, block)
                pair.append(block)
            blocks.append(pair)
        return blocks

    def put_main(out_high, held, take):
        real, imag = held[take // 2]
        if take % 2:
            main = jnp.where(first, roll(real, half), imag)
        else:
            main = jnp.where(first, real, roll(imag, half))
        send[out_high * radix + take, :rows_hi] = main

    def put_extra(out_high, blocks, take):
        block = None
        for f in range(radix):
            re, im = mixers[take][f]
            term = re * blocks[f][0] + im * blocks[f][1]
            block = term if block is None else block + term
        own = (take % 2) * 2 + take // 2
        moved = [roll(block[rows_hi - tail :], 2 * group * (own - k)) for k in range(radix) if k != own]
        send[out_high * radix + take, rows_hi:] = jnp.where(
            outer[: rows_hi - tail] == own, jnp.concatenate(moved, axis=0), block[: rows_hi - tail]
        )

    def post(seat, level, rows):
        pltpu.make_async_remote_copy(
            src_ref=send.at[seat * radix + level, rows],
            dst_ref=recv.at[me, rows],
            send_sem=send_sem,
            recv_sem=recv_sem.at[n],
            device_id={"wide": seat, "narrow": level},
            device_id_type=MESH,
        ).start()

    def lowest(first_seat, rows):
        last_seat = first_seat + 1
        alone = (n == 0) & (lax.div(w, 2) == first_seat // 2)
        other_seat = first_seat + last_seat - w

        def body(seat, carry):
            post(seat, 0, rows)
            return carry

        lax.fori_loop(
            jnp.where(alone, other_seat, first_seat), jnp.where(alone, other_seat, last_seat) + 1, body, 0
        )

    whole = pl.ds(0, rows_all)

    def below(level, carry):
        for seat in seats:
            post(seat, level, whole)
        return carry

    def above(level, carry):
        pl.semaphore_wait(known.at[level], radix)
        return below(level, carry)

    early, opened = {}, {}
    for out_high in range(2):
        early[out_high] = merged(out_high)
        put_main(out_high, early[out_high], 0)
        opened[out_high] = transposed(early[out_high])
        put_extra(out_high, opened[out_high], 0)

    peers = radix - 1 - w

    @pl.when((n == 0) & (peers > 0))
    def _():
        pl.semaphore_wait(known.at[n], peers)

    lowest(0, whole)

    for out_high in (2, 3, 0, 1):
        if out_high in early:
            held, blocks = early[out_high], opened[out_high]
        else:
            held = merged(out_high)
            blocks = transposed(held)
        for take in range(1 if out_high in early else 0, radix):
            put_main(out_high, held, take)
            put_extra(out_high, blocks, take)

    def own_level():
        @pl.when(peers > 0)
        def _():
            pl.semaphore_wait(known.at[n], peers)

        for seat in seats[:-1]:
            post(seat, n, whole)

    lowest(2, whole)

    @pl.when(n == 2)
    def _():
        own_level()
        above(3, 0)

    lax.fori_loop(1, n, below, 0)

    @pl.when((n == 1) | (n == 3))
    def _():
        own_level()

    lax.fori_loop(jnp.where(n == 2, radix, n + 1), radix, above, 0)
    recv[me] = send[w * radix + n]

    for begin in range(slots, total_pairs, slots):
        gate.update(merge(order[begin : begin + slots]))
    low = kron_all([gate[pair] for pair in range(start - 2, -1, -1)])
    block = jnp.concatenate(
        [jnp.concatenate([low[0], low[1]], axis=1), jnp.concatenate([-low[1], low[0]], axis=1)], axis=0
    )
    block = jnp.concatenate([jnp.concatenate([block] * radix, axis=0)] * radix, axis=1)
    down = lax.broadcasted_iota(jnp.int32, (LANES, LANES), 0)
    across = lax.broadcasted_iota(jnp.int32, (LANES, LANES), 1)
    grouped = jnp.where(down // (2 * group) == across // (2 * group), block, 0.0).T
    parts = kron_all([gate[pair] for pair in range(start - 1, -1, -1)])
    plain = jnp.concatenate(
        [jnp.concatenate([parts[0], parts[1]], axis=1), jnp.concatenate([-parts[1], parts[0]], axis=1)],
        axis=0,
    ).T
    for index, item in enumerate((plain, grouped)):
        lane_hi[index], lane_lo[index] = split(item)
    row_members = [gate[pair] for pair in range(total_pairs - 1, start + 1, -1)]
    for index, item in enumerate(kron_all(row_members)):
        for at, held in enumerate(split(item)):
            into = (row_hi, row_lo)[at]
            for source in range(count):
                place = (source % radix) * radix + source // radix
                into[index, place * rows_hi : (place + 1) * rows_hi] = held[source * rows_hi : (source + 1) * rows_hi]

    def settled(group, size):
        return pltpu.make_async_remote_copy(
            src_ref=send.at[pl.ds(0, size)],
            dst_ref=recv.at[pl.ds(0, size)],
            send_sem=send_sem,
            recv_sem=recv_sem.at[group],
            device_id={"wide": w, "narrow": n},
            device_id_type=MESH,
        )

    settled(0, count - 1).wait_send()
    settled(n, radix - 1).wait_recv()
    for step in range(1, radix):
        settled(lax.rem(n + step, radix), radix).wait_recv()


def finish_kernel(radix, recv, lane_hi, lane_lo, row_hi, row_lo, out_hbm, marg_hbm, fin, prob, marg, sems):
    rows_hi = recv.shape[1] * radix // (2 * radix - 1)
    tail = rows_hi // radix
    size = recv.shape[0] * rows_hi
    half = LANES // 2
    group = half // radix
    blocks = size // LANES
    rows = (row_hi[0], row_lo[0]), (row_hi[1], row_lo[1])

    def apply(which, value, keep):
        held = split(value.reshape(size, LANES))
        turned = dot((lane_hi[which], lane_lo[which]), held, 1)
        turned = split(turned[:keep])
        return dot(turned, rows[0], 0), dot(turned, rows[1], 0)

    with_real, with_imag = apply(0, recv[:, :rows_hi], LANES)
    real = with_real[:half] - with_imag[half:]
    imag = with_real[half:] + with_imag[:half]
    for block in range(blocks):
        columns = slice(block * LANES, (block + 1) * LANES)
        fin[pl.ds(block * 2, half, stride=2 * blocks), :] = real[:, columns]
        fin[pl.ds(block * 2 + 1, half, stride=2 * blocks), :] = imag[:, columns]
    out_copy = pltpu.make_async_copy(fin, out_hbm, sems.at[0])
    out_copy.start()
    density = real * real + imag * imag
    for index in range(radix):
        prob[index] = density[index * group : (index + 1) * group]
    packed = recv[:, rows_hi:]
    outer = lax.broadcasted_iota(jnp.int32, (1, tail, LANES), 2) // (2 * group)
    n = lax.axis_index("narrow")
    own = (n % 2) * 2 + n // 2
    last = packed[:, :tail]
    for index in range(radix - 1):
        kept = index + jnp.where(own <= index, 1, 0)
        piece = packed[:, index * tail : (index + 1) * tail]
        piece = pltpu.roll(piece, lax.rem(2 * group * (kept - own) + LANES, LANES), 2)
        last = jnp.where(outer == kept, piece, last)
    wide = jnp.concatenate([packed, last], axis=1)
    with_real, with_imag = apply(1, wide, LANES)
    total = prob[n]
    for index in range(radix):
        at = 2 * group * index
        real = with_real[at : at + group] - with_imag[at + group : at + 2 * group]
        imag = with_real[at + group : at + 2 * group] + with_imag[at : at + group]
        total = total + jnp.where(own == index, 0.0, real * real + imag * imag)
    for block in range(blocks):
        marg[pl.ds(block, group, stride=blocks), :] = total[:, block * LANES : (block + 1) * LANES]
    marg_copy = pltpu.make_async_copy(marg, marg_hbm, sems.at[1])
    marg_copy.start()
    out_copy.wait()
    marg_copy.wait()


def window_plan(wide_count, narrow_count, amplitudes, gates_shape):
    layers, pairs, radix = gates_shape[0], gates_shape[1], gates_shape[-1]
    high_bits = (wide_count * narrow_count).bit_length() - 1
    local_bits = amplitudes.bit_length() - 1
    total_bits = high_bits + local_bits
    if high_bits % 2 or local_bits % 2 or wide_count != radix or narrow_count != radix:
        return None
    if 2 * pairs != local_bits:
        return None
    offset = ((layers - 1) * high_bits) % total_bits
    start = offset // 2 - high_bits // 2
    if layers & (layers - 1) or LANES % (layers * radix) or start < 2 or LANES < 3 * layers * radix or offset // 2 >= pairs or 2 * radix**start != LANES:
        return None
    rows_hi = radix ** (pairs - offset // 2)
    if rows_hi % 8:
        return None
    for which in range(total_bits // 2):
        if all((which - layer * (high_bits // 2)) % (total_bits // 2) >= pairs for layer in range(layers)):
            return None
    return (layers, pairs, high_bits // 2, total_bits // 2, start, radix), rows_hi


def merged_local(plan, rows_hi, state, gates):
    radix = plan[-1]
    amplitudes = state.shape[-1]
    rows = amplitudes // LANES
    count = radix * radix
    own = amplitudes // radix // LANES
    x = jnp.swapaxes(state.reshape(2, rows, LANES), 0, 1).reshape(2 * rows, LANES)
    g = jnp.transpose(gates, (1, 2, 3, 4, 0)).reshape(-1, radix, gates.shape[0])
    f32, bf16 = jnp.float32, jnp.bfloat16
    size = count * rows_hi
    message = 2 * rows_hi - rows_hi // radix
    shared = (
        pltpu.VMEM((count, message, LANES), f32),
        pltpu.VMEM((2, LANES, LANES), bf16),
        pltpu.VMEM((2, LANES, LANES), bf16),
        pltpu.VMEM((2, size, size), bf16),
        pltpu.VMEM((2, size, size), bf16),
    )
    held = pl.pallas_call(
        functools.partial(exchange_kernel, plan),
        out_shape=shared,
        in_specs=[pl.BlockSpec(memory_space=pltpu.HBM)] * 2,
        out_specs=[pl.BlockSpec(memory_space=pltpu.VMEM)] * len(shared),
        scratch_shapes=[
            pltpu.VMEM(x.shape, f32),
            pltpu.VMEM(g.shape, f32),
            pltpu.VMEM((count, message, LANES), f32),
            pltpu.SemaphoreType.DMA((2,)),
            pltpu.SemaphoreType.DMA,
            pltpu.SemaphoreType.DMA((radix,)),
            pltpu.SemaphoreType.REGULAR((radix,)),
        ],
        compiler_params=pltpu.CompilerParams(
            collective_id=0, has_side_effects=True, vmem_limit_bytes=8 * 2**20
        ),
        name="exchange",
    )(
        pltpu.with_memory_space_constraint(x, pltpu.HBM),
        pltpu.with_memory_space_constraint(g, pltpu.HBM),
    )
    out, marg = pl.pallas_call(
        functools.partial(finish_kernel, radix),
        out_shape=(pltpu.HBM((2 * rows, LANES), f32), pltpu.HBM((own, LANES), f32)),
        in_specs=[pl.BlockSpec(memory_space=pltpu.VMEM)] * len(shared),
        out_specs=[pl.BlockSpec(memory_space=pltpu.HBM)] * 2,
        scratch_shapes=[
            pltpu.VMEM((2 * rows, LANES), f32),
            pltpu.VMEM((radix, LANES // 2 // radix, size), f32),
            pltpu.VMEM((own, LANES), f32),
            pltpu.SemaphoreType.DMA((2,)),
        ],
        compiler_params=pltpu.CompilerParams(vmem_limit_bytes=8 * 2**20),
        name="finish",
    )(*held)
    final = jnp.swapaxes(out.reshape(rows, 2, LANES), 0, 1).reshape(1, 1, 2, amplitudes)
    return final, marg.reshape(1, -1)


def local(state, gates):
    wide_count = lax.axis_size("wide")
    narrow_count = lax.axis_size("narrow")
    amplitudes = state.shape[-1]
    found = window_plan(wide_count, narrow_count, amplitudes, gates.shape)
    if found is not None:
        return merged_local(*found, state, gates)
    flat = state.reshape(2, amplitudes)
    for layer_index in range(gates.shape[0]):
        if layer_index > 0:
            flat = rotate(flat, wide_count, narrow_count)
        flat = apply_layer(flat, gates[layer_index])
    prob = flat[0] * flat[0] + flat[1] * flat[1]
    marginal = lax.psum_scatter(prob, "narrow", scatter_dimension=0, tiled=True)
    return (flat.reshape(1, 1, 2, amplitudes), marginal.reshape(1, -1))


def solution(mesh):
    in_specs = (P(("slices", "wide"), "narrow", None, None), P())
    out_specs = (P(("slices", "wide"), "narrow", None, None), P(("slices", "wide"), "narrow"))
    return jax.shard_map(local, mesh=mesh, in_specs=in_specs, out_specs=out_specs, check_vma=False)
```

```python
import functools

import jax
import jax.numpy as jnp
from jax import lax
from jax.experimental import pallas as pl
from jax.experimental.pallas import tpu as pltpu
from jax.sharding import PartitionSpec as P


def kron_chain(members):
    real_part = members[0][0]
    imag_part = members[0][1]
    for member in members[1:]:
        other_real = member[0]
        other_imag = member[1]
        new_real = jnp.kron(real_part, other_real) - jnp.kron(imag_part, other_imag)
        new_imag = jnp.kron(real_part, other_imag) + jnp.kron(imag_part, other_real)
        real_part, imag_part = (new_real, new_imag)
    return (real_part, imag_part)


def rotate(flat, wide_count, narrow_count):
    devices = wide_count * narrow_count
    amplitudes = flat.shape[1]
    rest = amplitudes // devices
    blocks = flat.reshape(2, rest, devices)
    turned = jnp.swapaxes(blocks, 1, 2)
    moved = lax.all_to_all(turned, ("wide", "narrow"), split_axis=1, concat_axis=1, tiled=True)
    return moved.reshape(2, amplitudes)


def apply_layer(flat, layer_gates):
    amplitudes = flat.shape[1]
    pairs = layer_gates.shape[0]
    upper = amplitudes // 256
    low_real, low_imag = kron_chain([layer_gates[index] for index in range(3, -1, -1)])
    high_real, high_imag = kron_chain([layer_gates[index] for index in range(pairs - 1, 3, -1)])
    blocks = flat.reshape(2, upper, 256)
    real_rows = blocks[0]
    imag_rows = blocks[1]
    highest = lax.Precision.HIGHEST
    next_real = jnp.dot(real_rows, low_real.T, precision=highest) - jnp.dot(
        imag_rows, low_imag.T, precision=highest
    )
    next_imag = jnp.dot(real_rows, low_imag.T, precision=highest) + jnp.dot(
        imag_rows, low_real.T, precision=highest
    )
    final_real = jnp.dot(high_real, next_real, precision=highest) - jnp.dot(
        high_imag, next_imag, precision=highest
    )
    final_imag = jnp.dot(high_imag, next_real, precision=highest) + jnp.dot(
        high_real, next_imag, precision=highest
    )
    return jnp.stack([final_real, final_imag]).reshape(2, amplitudes)


MESH = pl.DeviceIdType.MESH
LANES = 128


def complex_mul(left, right):
    return (
        left[0] * right[0] - left[1] * right[1],
        left[0] * right[1] + left[1] * right[0],
    )


def take_lanes(value, source):
    return jnp.take_along_axis(value, source, axis=1, mode="promise_in_bounds")


def gate_tools(g, plan):
    layers, pairs, shift, total_pairs, _, radix = plan
    shape = (2 * radix, LANES)
    lane = lax.broadcasted_iota(jnp.int32, shape, 1)
    down = lax.broadcasted_iota(jnp.int32, shape, 0)
    width = radix * layers
    layer, row, slot = lane % layers, (lane // layers) % radix, lane // width
    pad = jnp.zeros((radix, LANES - layers), jnp.float32)
    tiles, planes = [], []
    for pair in range(pairs):
        tiles.append([])
        plane = None
        for at in range(radix):
            tile = jnp.concatenate(
                [jnp.concatenate([g[(pair * 2 + c) * radix + at], pad], axis=1) for c in range(2)], axis=0
            )
            tiles[-1].append(tile)
            tile = take_lanes(tile, layer)
            plane = tile if plane is None else jnp.where(row == at, tile, plane)
        planes.append(plane)
    sign = jnp.where(down < radix, -1.0, 1.0)

    def merge(held, direct=False):
        place = held[0] - shift * layer
        for index, pair in enumerate(held[1:]):
            place = jnp.where(slot == index + 1, pair - shift * layer, place)
        for _ in range(-(-layers * shift // total_pairs)):
            place = jnp.where(place < 0, place + total_pairs, place)
        total = jnp.where(down == row, 1.0, 0.0)
        for pair in range(pairs):
            total = jnp.where(place == pair, planes[pair], total)
        step = 1
        while step < layers:
            before = jnp.maximum(layer - step, 0)
            straight, crossed = None, None
            for at in range(radix):
                if direct and step == 1:
                    early = jnp.where(down == at, 1.0, 0.0)
                    previous = jnp.where(place + shift < total_pairs, place + shift, place + shift - total_pairs)
                    for pair in range(pairs):
                        early = jnp.where(previous == pair, take_lanes(tiles[pair][at], before), early)
                else:
                    early = take_lanes(total, slot * width + at * layers + before)
                one_part = total[at : at + 1] * early
                two_part = total[radix + at : radix + at + 1] * early
                straight = one_part if straight is None else straight + one_part
                crossed = two_part if crossed is None else crossed + two_part
            total = straight + sign * pltpu.roll(crossed, radix, 0)
            step *= 2
        return {
            pair: [
                take_lanes(total, jnp.full(shape, index * width + (at + 1) * layers - 1, jnp.int32))
                for at in range(radix)
            ]
            for index, pair in enumerate(held)
        }

    return merge


def kron_all(members):
    radix = len(members[0])
    size = radix ** len(members)
    width = max(size, LANES)
    lane = lax.broadcasted_iota(jnp.int32, (2 * radix, width), 1)
    rows = None
    for place, member in enumerate(reversed(members)):
        field = (lane // radix**place) % radix
        columns = [jnp.concatenate([column] * (width // LANES), axis=1) for column in member]
        spread = columns[-1]
        for index in range(radix - 1):
            spread = jnp.where(field == index, columns[index], spread)
        wide = spread[:radix], spread[radix:]
        if rows is None:
            rows = wide
            continue
        pieces = [
            complex_mul(tuple(part[index : index + 1, :] for part in wide), rows)
            for index in range(radix)
        ]
        rows = tuple(jnp.concatenate([piece[c] for piece in pieces], axis=0) for c in range(2))
    return tuple(part[:, :size] for part in rows)


def split(value):
    high = value.astype(jnp.bfloat16)
    return high, (value - high.astype(jnp.float32)).astype(jnp.bfloat16)


def precise(left, right, contract):
    def one(a, b):
        return lax.dot_general(a, b, (((1,), (contract,)), ((), ())), preferred_element_type=jnp.float32)

    return one(left[0], right[0]) + (one(left[0], right[1]) + one(left[1], right[0]))


def precise_one(a, b):
    return lax.dot_general(a, b, (((1,), (0,)), ((), ())), preferred_element_type=jnp.float32)


def pairs_of(n):
    near = n, jnp.where(n == 0, 1, n - 1)
    return near, (jnp.where(n < 2, 2, 0), jnp.where(n < 3, 3, 1))


def contribution(radix, recv, lanes, rows, levels, n):
    held = jnp.concatenate([recv[pl.ds(level * radix, radix)] for level in levels], axis=0)
    rows_hi = held.shape[1] * radix // (2 * radix - 1)
    tail = rows_hi // radix
    size = held.shape[0] * rows_hi
    wide = LANES // radix
    packed = held[:, rows_hi:]
    outer = lax.broadcasted_iota(jnp.int32, (1, tail, LANES), 2) // wide
    own = (n % 2) * 2 + n // 2
    last = packed[:, :tail]
    for index in range(radix - 1):
        kept = index + jnp.where(own <= index, 1, 0)
        piece = packed[:, index * tail : (index + 1) * tail]
        piece = pltpu.roll(piece, lax.rem(wide * (kept - own) + LANES, LANES), 2)
        last = jnp.where(outer == kept, piece, last)
    turned = []
    for which, value in enumerate((held[:, :rows_hi], jnp.concatenate([packed, last], axis=1))):
        item = precise(tuple(part[which] for part in lanes), split(value.reshape(size, LANES)), 1)
        turned.append(jnp.concatenate([item[: LANES // 2], item[LANES // 2 :]], axis=1))
    matrix = [
        jnp.concatenate([part[c, level] for c in range(2) for level in levels], axis=0) for part in rows
    ]
    high, low = split(jnp.concatenate(turned, axis=0))
    both = precise_one(jnp.concatenate([high, low], axis=0), matrix[0])
    rows = high.shape[0]
    return both[:rows] + (both[rows:] + precise_one(high, matrix[1]))


def greet(semaphore, seat, level):
    pl.semaphore_signal(semaphore, inc=1, device_id={"wide": seat, "narrow": level}, device_id_type=MESH)


def exchange_kernel(plan, x_hbm, g_hbm, recv, acc, lane_hi, lane_lo, row_hi, row_lo, x, g, send,
                    local_sem, send_sem, recv_sem, known):
    layers, pairs, shift, total_pairs, start, radix = plan
    w = lax.axis_index("wide")
    n = lax.axis_index("narrow")
    me = n * radix + w
    count = radix * radix

    barrier = pltpu.get_barrier_semaphore()
    copy_g = pltpu.make_async_copy(g_hbm, g, local_sem.at[0])
    copy_x = pltpu.make_async_copy(x_hbm, x, local_sem.at[1])
    copy_g.start()
    copy_x.start()
    row, core = lax.div(w, 2), lax.rem(w, 2)
    other = 2 * (1 - row)
    seats = [other + core, other + 1 - core, 2 * row + 1 - core, w]
    for seat in range(1, radix):
        @pl.when(seat > w)
        def _():
            greet(barrier, seat, n)

    for level in range(1, radix):
        @pl.when(level > n)
        def _():
            for seat in range(radix):
                greet(barrier, seat, level)

    @pl.when(me > 0)
    def _():
        pl.semaphore_wait(barrier, me)

    for level in range(radix - 2, -1, -1):
        @pl.when(level < n)
        def _():
            for seat in range(radix):
                greet(known.at[n, row], seat, level)

    for seat in range(radix - 1):
        @pl.when(seat < w)
        def _():
            greet(known.at[n, row], seat, n)

    copy_g.wait()
    copy_x.wait()

    merge = gate_tools(g, plan)
    order = list(range(start - 1, start + 2)) + list(range(start - 1)) + list(range(start + 2, total_pairs))
    slots = LANES // (radix * layers)
    gate = merge(order[:slots], True)
    split_gate, low_gate, high_gate = (gate[pair] for pair in range(start - 1, start + 2))

    half = LANES // 2
    group = half // radix
    rows_all = send.shape[1]
    rows_hi = rows_all * radix // (2 * radix - 1)
    tail = rows_hi // radix
    shape = (rows_hi, LANES)
    lane = lax.broadcasted_iota(jnp.int32, shape, 1)
    first = lane < half
    field = (lane // group) % radix
    outer = lane // (2 * group)

    def entry(gate, row, column):
        return tuple(
            jnp.broadcast_to(gate[row][at : at + 1], shape) for at in (column, column + radix)
        )

    def both(gate, one, other):
        return tuple(jnp.where(first, a, b) for a, b in zip(entry(gate, *one), entry(gate, *other)))

    def add(total, term):
        return term if total is None else (total[0] + term[0], total[1] + term[1])

    def roll(value, amount):
        amount %= LANES
        return pltpu.roll(value, amount, 1) if amount else value

    same = [[both(low_gate, (2 * o, 2 * i), (2 * o + 1, 2 * i + 1)) for i in range(2)] for o in range(2)]
    cross = [[both(low_gate, (2 * o, 2 * i + 1), (2 * o + 1, 2 * i)) for i in range(2)] for o in range(2)]
    stage = []
    stride = 4 * radix
    for high in range(radix):
        held = []
        for i in range(2):
            held.append(tuple(x[pl.ds(high * 4 + i * 2 + c, rows_hi, stride=stride), :] for c in range(2)))
        turned = [tuple(roll(v, half) for v in pair) for pair in held]
        result = []
        for o in range(2):
            total = None
            for i in range(2):
                total = add(total, complex_mul(same[o][i], held[i]))
                total = add(total, complex_mul(cross[o][i], turned[i]))
            result.append(total)
        stage.append(result)
    sign = jnp.where(field % 2 == 0, -1.0, 1.0)
    mixers = [[entry(split_gate, take, f) for f in range(radix)] for take in range(radix)]
    mixers = [[(re, im * sign) for re, im in line] for line in mixers]

    def merged(out_high):
        coefs = [entry(high_gate, out_high, high) for high in range(radix)]
        held = []
        for o in range(2):
            total = None
            for high in range(radix):
                total = add(total, complex_mul(coefs[high], stage[high][o]))
            held.append(total)
        return held

    def transposed(held):
        turned = {}
        for o in range(2):
            for c in range(2):
                for d in range(2 * o - 3, 2 * o + 2):
                    turned[o, c, d] = roll(held[o][c], d * group)
        blocks = []
        for f in range(radix):
            pair = []
            for flip in range(2):
                block = None
                for o in range(2):
                    for c in range(2):
                        piece = turned[o, c ^ flip, 2 * o + c - f]
                        block = piece if block is None else jnp.where(field == 2 * o + c, piece, block)
                pair.append(block)
            blocks.append(pair)
        return blocks

    def put_main(out_high, held, take):
        real, imag = held[take // 2]
        if take % 2:
            main = jnp.where(first, roll(real, half), imag)
        else:
            main = jnp.where(first, real, roll(imag, half))
        send[out_high * radix + take, :rows_hi] = main

    def put_extra(out_high, blocks, take):
        block = None
        for f in range(radix):
            re, im = mixers[take][f]
            term = re * blocks[f][0] + im * blocks[f][1]
            block = term if block is None else block + term
        own = (take % 2) * 2 + take // 2
        moved = [roll(block[rows_hi - tail :], 2 * group * (own - k)) for k in range(radix) if k != own]
        send[out_high * radix + take, rows_hi:] = jnp.where(
            outer[: rows_hi - tail] == own, jnp.concatenate(moved, axis=0), block[: rows_hi - tail]
        )

    def post(seat, level, rows):
        pltpu.make_async_remote_copy(
            src_ref=send.at[seat * radix + level, rows],
            dst_ref=recv.at[me, rows],
            send_sem=send_sem,
            recv_sem=recv_sem.at[n],
            device_id={"wide": seat, "narrow": level},
            device_id_type=MESH,
        ).start()

    def lowest(first_seat, rows):
        last_seat = first_seat + 1
        alone = (n == 0) & (lax.div(w, 2) == first_seat // 2)
        other_seat = first_seat + last_seat - w

        def body(seat, carry):
            post(seat, 0, rows)
            return carry

        lax.fori_loop(
            jnp.where(alone, other_seat, first_seat), jnp.where(alone, other_seat, last_seat) + 1, body, 0
        )

    whole = pl.ds(0, rows_all)

    def below(level, carry):
        for seat in seats:
            post(seat, level, whole)
        return carry

    def above(level, carry):
        for side, pair in ((row, seats[2:]), (1 - row, seats[:2])):
            pl.semaphore_wait(known.at[level, side], 2)
            for seat in pair:
                post(seat, level, whole)
        return carry

    early, opened = {}, {}
    for out_high in range(2):
        early[out_high] = merged(out_high)
        put_main(out_high, early[out_high], 0)
        opened[out_high] = transposed(early[out_high])
        put_extra(out_high, opened[out_high], 0)

    def meet():
        @pl.when(core == 0)
        def _():
            pl.semaphore_wait(known.at[n, row], 1)

        @pl.when(row == 0)
        def _():
            pl.semaphore_wait(known.at[n, 1], 2)


    @pl.when(n == 0)
    def _():
        meet()

    lowest(0, whole)

    for out_high in (2, 3, 0, 1):
        if out_high in early:
            held, blocks = early[out_high], opened[out_high]
        else:
            held = merged(out_high)
            blocks = transposed(held)
        for take in range(1 if out_high in early else 0, radix):
            put_main(out_high, held, take)
            put_extra(out_high, blocks, take)

    def own_level():
        meet()
        for seat in seats[:-1]:
            post(seat, n, whole)

    lowest(2, whole)

    @pl.when(n == 2)
    def _():
        own_level()
        above(3, 0)

    lax.fori_loop(1, n, below, 0)

    @pl.when((n == 1) | (n == 3))
    def _():
        own_level()

    lax.fori_loop(jnp.where(n == 2, radix, n + 1), radix, above, 0)
    recv[me] = send[w * radix + n]

    for begin in range(slots, total_pairs, slots):
        gate.update(merge(order[begin : begin + slots]))
    low = kron_all([gate[pair] for pair in range(start - 2, -1, -1)])
    block = jnp.concatenate(
        [jnp.concatenate([low[0], low[1]], axis=1), jnp.concatenate([-low[1], low[0]], axis=1)], axis=0
    )
    block = jnp.concatenate([jnp.concatenate([block] * radix, axis=0)] * radix, axis=1)
    down = lax.broadcasted_iota(jnp.int32, (LANES, LANES), 0)
    across = lax.broadcasted_iota(jnp.int32, (LANES, LANES), 1)
    grouped = jnp.where(down // (2 * group) == across // (2 * group), block, 0.0).T
    parts = kron_all([gate[pair] for pair in range(start - 1, -1, -1)])
    plain = jnp.concatenate(
        [jnp.concatenate([parts[0], parts[1]], axis=1), jnp.concatenate([-parts[1], parts[0]], axis=1)],
        axis=0,
    ).T
    stripes = range(0, LANES, 2 * group)
    grouped = jnp.concatenate(
        [grouped[at + shift : at + shift + group] for shift in (0, group) for at in stripes], axis=0
    )
    for index, item in enumerate((plain, grouped)):
        lane_hi[index], lane_lo[index] = split(item)
    row_members = [gate[pair] for pair in range(total_pairs - 1, start + 1, -1)]
    real, imag = (split(item) for item in kron_all(row_members))
    for at, into in enumerate((row_hi, row_lo)):
        for source in range(count):
            seat, level = source // radix, source % radix
            rows = slice(source * rows_hi, (source + 1) * rows_hi)
            place = slice(seat * rows_hi, (seat + 1) * rows_hi)
            into[0, level, place] = jnp.concatenate([real[at][rows], imag[at][rows]], axis=1)
            into[1, level, place] = jnp.concatenate([-imag[at][rows], real[at][rows]], axis=1)

    def settled(group, size):
        return pltpu.make_async_remote_copy(
            src_ref=send.at[pl.ds(0, size)],
            dst_ref=recv.at[pl.ds(0, size)],
            send_sem=send_sem,
            recv_sem=recv_sem.at[group],
            device_id={"wide": w, "narrow": n},
            device_id_type=MESH,
        )

    near, far = pairs_of(n)
    settled(near[0], radix - 1).wait_recv()
    settled(near[1], radix).wait_recv()
    acc[...] = contribution(radix, recv, (lane_hi, lane_lo), (row_hi, row_lo), near, n)
    settled(0, count - 1).wait_send()
    for level in far:
        settled(level, radix).wait_recv()


def finish_kernel(radix, recv, acc, lane_hi, lane_lo, row_hi, row_lo, out_hbm, marg_hbm, fin, prob, marg, sems):
    half = LANES // 2
    group = half // radix
    size = acc.shape[1] // 2
    blocks = size // LANES
    n = lax.axis_index("narrow")
    own = (n % 2) * 2 + n // 2
    total = acc[...] + contribution(radix, recv, (lane_hi, lane_lo), (row_hi, row_lo), pairs_of(n)[1], n)
    real, imag = total[:, :size], total[:, size:]
    for block in range(blocks):
        columns = slice(block * LANES, (block + 1) * LANES)
        fin[pl.ds(block * 2, half, stride=2 * blocks), :] = real[:half, columns]
        fin[pl.ds(block * 2 + 1, half, stride=2 * blocks), :] = imag[:half, columns]
    out_copy = pltpu.make_async_copy(fin, out_hbm, sems.at[0])
    out_copy.start()
    density = real * real + imag * imag
    for index in range(radix):
        prob[index] = density[index * group : (index + 1) * group]
    total = prob[n]
    for index in range(radix):
        at = half + group * index
        total = total + jnp.where(own == index, 0.0, density[at : at + group])
    for block in range(blocks):
        marg[pl.ds(block, group, stride=blocks), :] = total[:, block * LANES : (block + 1) * LANES]
    marg_copy = pltpu.make_async_copy(marg, marg_hbm, sems.at[1])
    marg_copy.start()
    out_copy.wait()
    marg_copy.wait()


def window_plan(wide_count, narrow_count, amplitudes, gates_shape):
    layers, pairs, radix = gates_shape[0], gates_shape[1], gates_shape[-1]
    high_bits = (wide_count * narrow_count).bit_length() - 1
    local_bits = amplitudes.bit_length() - 1
    total_bits = high_bits + local_bits
    if high_bits % 2 or local_bits % 2 or wide_count != radix or narrow_count != radix:
        return None
    if 2 * pairs != local_bits:
        return None
    offset = ((layers - 1) * high_bits) % total_bits
    start = offset // 2 - high_bits // 2
    if layers & (layers - 1) or LANES % (layers * radix) or start < 2 or LANES < 3 * layers * radix or offset // 2 >= pairs or 2 * radix**start != LANES:
        return None
    rows_hi = radix ** (pairs - offset // 2)
    if rows_hi % 8:
        return None
    for which in range(total_bits // 2):
        if all((which - layer * (high_bits // 2)) % (total_bits // 2) >= pairs for layer in range(layers)):
            return None
    return (layers, pairs, high_bits // 2, total_bits // 2, start, radix), rows_hi


def merged_local(plan, rows_hi, state, gates):
    radix = plan[-1]
    amplitudes = state.shape[-1]
    rows = amplitudes // LANES
    count = radix * radix
    own = amplitudes // radix // LANES
    x = jnp.swapaxes(state.reshape(2, rows, LANES), 0, 1).reshape(2 * rows, LANES)
    g = jnp.transpose(gates, (1, 2, 3, 4, 0)).reshape(-1, radix, gates.shape[0])
    f32, bf16 = jnp.float32, jnp.bfloat16
    size = count * rows_hi
    message = 2 * rows_hi - rows_hi // radix
    shared = (
        pltpu.VMEM((count, message, LANES), f32),
        pltpu.VMEM((LANES, 2 * size), f32),
        pltpu.VMEM((2, LANES, LANES), bf16),
        pltpu.VMEM((2, LANES, LANES), bf16),
        pltpu.VMEM((2, radix, size // radix, 2 * size), bf16),
        pltpu.VMEM((2, radix, size // radix, 2 * size), bf16),
    )
    held = pl.pallas_call(
        functools.partial(exchange_kernel, plan),
        out_shape=shared,
        in_specs=[pl.BlockSpec(memory_space=pltpu.HBM)] * 2,
        out_specs=[pl.BlockSpec(memory_space=pltpu.VMEM)] * len(shared),
        scratch_shapes=[
            pltpu.VMEM(x.shape, f32),
            pltpu.VMEM(g.shape, f32),
            pltpu.VMEM((count, message, LANES), f32),
            pltpu.SemaphoreType.DMA((2,)),
            pltpu.SemaphoreType.DMA,
            pltpu.SemaphoreType.DMA((radix,)),
            pltpu.SemaphoreType.REGULAR((radix, 2)),
        ],
        compiler_params=pltpu.CompilerParams(
            collective_id=0, has_side_effects=True, vmem_limit_bytes=8 * 2**20
        ),
        name="exchange",
    )(
        pltpu.with_memory_space_constraint(x, pltpu.HBM),
        pltpu.with_memory_space_constraint(g, pltpu.HBM),
    )
    out, marg = pl.pallas_call(
        functools.partial(finish_kernel, radix),
        out_shape=(pltpu.HBM((2 * rows, LANES), f32), pltpu.HBM((own, LANES), f32)),
        in_specs=[pl.BlockSpec(memory_space=pltpu.VMEM)] * len(shared),
        out_specs=[pl.BlockSpec(memory_space=pltpu.HBM)] * 2,
        scratch_shapes=[
            pltpu.VMEM((2 * rows, LANES), f32),
            pltpu.VMEM((radix, LANES // 2 // radix, size), f32),
            pltpu.VMEM((own, LANES), f32),
            pltpu.SemaphoreType.DMA((2,)),
        ],
        compiler_params=pltpu.CompilerParams(vmem_limit_bytes=8 * 2**20),
        name="finish",
    )(*held)
    final = jnp.swapaxes(out.reshape(rows, 2, LANES), 0, 1).reshape(1, 1, 2, amplitudes)
    return final, marg.reshape(1, -1)


def local(state, gates):
    wide_count = lax.axis_size("wide")
    narrow_count = lax.axis_size("narrow")
    amplitudes = state.shape[-1]
    found = window_plan(wide_count, narrow_count, amplitudes, gates.shape)
    if found is not None:
        return merged_local(*found, state, gates)
    flat = state.reshape(2, amplitudes)
    for layer_index in range(gates.shape[0]):
        if layer_index > 0:
            flat = rotate(flat, wide_count, narrow_count)
        flat = apply_layer(flat, gates[layer_index])
    prob = flat[0] * flat[0] + flat[1] * flat[1]
    marginal = lax.psum_scatter(prob, "narrow", scatter_dimension=0, tiled=True)
    return (flat.reshape(1, 1, 2, amplitudes), marginal.reshape(1, -1))


def solution(mesh):
    in_specs = (P(("slices", "wide"), "narrow", None, None), P())
    out_specs = (P(("slices", "wide"), "narrow", None, None), P(("slices", "wide"), "narrow"))
    return jax.shard_map(local, mesh=mesh, in_specs=in_specs, out_specs=out_specs, check_vma=False)
```

```python
import functools

import jax
import jax.numpy as jnp
from jax import lax
from jax.experimental import pallas as pl
from jax.experimental.pallas import tpu as pltpu
from jax.sharding import PartitionSpec as P


def kron_chain(members):
    real_part = members[0][0]
    imag_part = members[0][1]
    for member in members[1:]:
        other_real = member[0]
        other_imag = member[1]
        new_real = jnp.kron(real_part, other_real) - jnp.kron(imag_part, other_imag)
        new_imag = jnp.kron(real_part, other_imag) + jnp.kron(imag_part, other_real)
        real_part, imag_part = (new_real, new_imag)
    return (real_part, imag_part)


def rotate(flat, wide_count, narrow_count):
    devices = wide_count * narrow_count
    amplitudes = flat.shape[1]
    rest = amplitudes // devices
    blocks = flat.reshape(2, rest, devices)
    turned = jnp.swapaxes(blocks, 1, 2)
    moved = lax.all_to_all(turned, ("wide", "narrow"), split_axis=1, concat_axis=1, tiled=True)
    return moved.reshape(2, amplitudes)


def apply_layer(flat, layer_gates):
    amplitudes = flat.shape[1]
    pairs = layer_gates.shape[0]
    upper = amplitudes // 256
    low_real, low_imag = kron_chain([layer_gates[index] for index in range(3, -1, -1)])
    high_real, high_imag = kron_chain([layer_gates[index] for index in range(pairs - 1, 3, -1)])
    blocks = flat.reshape(2, upper, 256)
    real_rows = blocks[0]
    imag_rows = blocks[1]
    highest = lax.Precision.HIGHEST
    next_real = jnp.dot(real_rows, low_real.T, precision=highest) - jnp.dot(
        imag_rows, low_imag.T, precision=highest
    )
    next_imag = jnp.dot(real_rows, low_imag.T, precision=highest) + jnp.dot(
        imag_rows, low_real.T, precision=highest
    )
    final_real = jnp.dot(high_real, next_real, precision=highest) - jnp.dot(
        high_imag, next_imag, precision=highest
    )
    final_imag = jnp.dot(high_imag, next_real, precision=highest) + jnp.dot(
        high_real, next_imag, precision=highest
    )
    return jnp.stack([final_real, final_imag]).reshape(2, amplitudes)


MESH = pl.DeviceIdType.MESH
LANES = 128


def complex_mul(left, right):
    return (
        left[0] * right[0] - left[1] * right[1],
        left[0] * right[1] + left[1] * right[0],
    )


def take_lanes(value, source):
    return jnp.take_along_axis(value, source, axis=1, mode="promise_in_bounds")


def gate_tools(g, plan):
    layers, pairs, shift, total_pairs, _, radix = plan
    shape = (2 * radix, LANES)
    lane = lax.broadcasted_iota(jnp.int32, shape, 1)
    down = lax.broadcasted_iota(jnp.int32, shape, 0)
    width = radix * layers
    layer, row, slot = lane % layers, (lane // layers) % radix, lane // width
    pad = jnp.zeros((radix, LANES - layers), jnp.float32)
    tiles, planes = [], []
    for pair in range(pairs):
        tiles.append([])
        plane = None
        for at in range(radix):
            tile = jnp.concatenate(
                [jnp.concatenate([g[(pair * 2 + c) * radix + at], pad], axis=1) for c in range(2)], axis=0
            )
            tiles[-1].append(tile)
            tile = take_lanes(tile, layer)
            plane = tile if plane is None else jnp.where(row == at, tile, plane)
        planes.append(plane)
    sign = jnp.where(down < radix, -1.0, 1.0)

    def merge(held, direct=False):
        place = held[0] - shift * layer
        for index, pair in enumerate(held[1:]):
            place = jnp.where(slot == index + 1, pair - shift * layer, place)
        for _ in range(-(-layers * shift // total_pairs)):
            place = jnp.where(place < 0, place + total_pairs, place)
        total = jnp.where(down == row, 1.0, 0.0)
        for pair in range(pairs):
            total = jnp.where(place == pair, planes[pair], total)
        step = 1
        while step < layers:
            before = jnp.maximum(layer - step, 0)
            straight, crossed = None, None
            for at in range(radix):
                if direct and step == 1:
                    early = jnp.where(down == at, 1.0, 0.0)
                    previous = jnp.where(place + shift < total_pairs, place + shift, place + shift - total_pairs)
                    for pair in range(pairs):
                        early = jnp.where(previous == pair, take_lanes(tiles[pair][at], before), early)
                else:
                    early = take_lanes(total, slot * width + at * layers + before)
                one_part = total[at : at + 1] * early
                two_part = total[radix + at : radix + at + 1] * early
                straight = one_part if straight is None else straight + one_part
                crossed = two_part if crossed is None else crossed + two_part
            total = straight + sign * pltpu.roll(crossed, radix, 0)
            step *= 2
        return {
            pair: [
                take_lanes(total, jnp.full(shape, index * width + (at + 1) * layers - 1, jnp.int32))
                for at in range(radix)
            ]
            for index, pair in enumerate(held)
        }

    return merge


def kron_all(members):
    radix = len(members[0])
    size = radix ** len(members)
    width = max(size, LANES)
    lane = lax.broadcasted_iota(jnp.int32, (2 * radix, width), 1)
    rows = None
    for place, member in enumerate(reversed(members)):
        field = (lane // radix**place) % radix
        columns = [jnp.concatenate([column] * (width // LANES), axis=1) for column in member]
        spread = columns[-1]
        for index in range(radix - 1):
            spread = jnp.where(field == index, columns[index], spread)
        wide = spread[:radix], spread[radix:]
        if rows is None:
            rows = wide
            continue
        pieces = [
            complex_mul(tuple(part[index : index + 1, :] for part in wide), rows)
            for index in range(radix)
        ]
        rows = tuple(jnp.concatenate([piece[c] for piece in pieces], axis=0) for c in range(2))
    return tuple(part[:, :size] for part in rows)


def split(value):
    high = value.astype(jnp.bfloat16)
    return high, (value - high.astype(jnp.float32)).astype(jnp.bfloat16)


def precise(left, right, contract):
    def one(a, b):
        return lax.dot_general(a, b, (((1,), (contract,)), ((), ())), preferred_element_type=jnp.float32)

    return one(left[0], right[0]) + (one(left[0], right[1]) + one(left[1], right[0]))


def precise_one(a, b):
    return lax.dot_general(a, b, (((1,), (0,)), ((), ())), preferred_element_type=jnp.float32)


def pairs_of(n):
    near = n, jnp.where(n == 0, 1, n - 1)
    return near, (jnp.where(n < 2, 2, 0), jnp.where(n < 3, 3, 1))


def contribution(radix, recv, lanes, rows, levels, n):
    held = jnp.concatenate([recv[pl.ds(level * radix, radix)] for level in levels], axis=0)
    rows_hi = held.shape[1] * radix // (2 * radix - 1)
    tail = rows_hi // radix
    size = held.shape[0] * rows_hi
    wide = LANES // radix
    packed = held[:, rows_hi:]
    outer = lax.broadcasted_iota(jnp.int32, (1, tail, LANES), 2) // wide
    own = (n % 2) * 2 + n // 2
    last = packed[:, :tail]
    for index in range(radix - 1):
        kept = index + jnp.where(own <= index, 1, 0)
        piece = packed[:, index * tail : (index + 1) * tail]
        piece = pltpu.roll(piece, lax.rem(wide * (kept - own) + LANES, LANES), 2)
        last = jnp.where(outer == kept, piece, last)
    turned = []
    for which, value in enumerate((held[:, :rows_hi], jnp.concatenate([packed, last], axis=1))):
        item = precise(tuple(part[which] for part in lanes), split(value.reshape(size, LANES)), 1)
        turned.append(jnp.concatenate([item[: LANES // 2], item[LANES // 2 :]], axis=1))
    matrix = [
        jnp.concatenate([part[c, level] for c in range(2) for level in levels], axis=0) for part in rows
    ]
    high, low = split(jnp.concatenate(turned, axis=0))
    both = precise_one(jnp.concatenate([high, low], axis=0), matrix[0])
    rows = high.shape[0]
    return both[:rows] + (both[rows:] + precise_one(high, matrix[1]))


def greet(semaphore, seat, level):
    pl.semaphore_signal(semaphore, inc=1, device_id={"wide": seat, "narrow": level}, device_id_type=MESH)


def exchange_kernel(plan, x_hbm, g_hbm, recv, acc, lane_hi, lane_lo, row_hi, row_lo, x, g, send,
                    local_sem, send_sem, recv_sem, known):
    layers, pairs, shift, total_pairs, start, radix = plan
    w = lax.axis_index("wide")
    n = lax.axis_index("narrow")
    me = n * radix + w
    count = radix * radix

    barrier = pltpu.get_barrier_semaphore()
    copy_g = pltpu.make_async_copy(g_hbm, g, local_sem.at[0])
    copy_x = pltpu.make_async_copy(x_hbm, x, local_sem.at[1])
    copy_g.start()
    copy_x.start()
    row, core = lax.div(w, 2), lax.rem(w, 2)
    other = 2 * (1 - row)
    seats = [other + core, other + 1 - core, 2 * row + 1 - core, w]
    for seat in range(1, radix):
        @pl.when(seat > w)
        def _():
            greet(barrier, seat, n)

    for level in range(1, radix):
        @pl.when(level > n)
        def _():
            for seat in range(radix):
                greet(barrier, seat, level)

    @pl.when(me > 0)
    def _():
        pl.semaphore_wait(barrier, me)

    for level in range(radix - 2, -1, -1):
        @pl.when(level < n)
        def _():
            for seat in range(radix):
                greet(known.at[n, row], seat, level)

    for seat in range(radix - 1):
        @pl.when(seat < w)
        def _():
            greet(known.at[n, row], seat, n)

    copy_g.wait()
    copy_x.wait()

    merge = gate_tools(g, plan)
    order = list(range(start - 1, start + 2)) + list(range(start - 1)) + list(range(start + 2, total_pairs))
    slots = LANES // (radix * layers)
    gate = merge(order[:slots], True)
    split_gate, low_gate, high_gate = (gate[pair] for pair in range(start - 1, start + 2))

    half = LANES // 2
    group = half // radix
    rows_all = send.shape[1]
    rows_hi = rows_all * radix // (2 * radix - 1)
    tail = rows_hi // radix
    shape = (rows_hi, LANES)
    lane = lax.broadcasted_iota(jnp.int32, shape, 1)
    first = lane < half
    field = (lane // group) % radix
    outer = lane // (2 * group)

    def entry(gate, row, column):
        return tuple(
            jnp.broadcast_to(gate[row][at : at + 1], shape) for at in (column, column + radix)
        )

    def both(gate, one, other):
        return tuple(jnp.where(first, a, b) for a, b in zip(entry(gate, *one), entry(gate, *other)))

    def add(total, term):
        return term if total is None else (total[0] + term[0], total[1] + term[1])

    def roll(value, amount):
        amount %= LANES
        return pltpu.roll(value, amount, 1) if amount else value

    same = [[both(low_gate, (2 * o, 2 * i), (2 * o + 1, 2 * i + 1)) for i in range(2)] for o in range(2)]
    cross = [[both(low_gate, (2 * o, 2 * i + 1), (2 * o + 1, 2 * i)) for i in range(2)] for o in range(2)]
    helds, stage = [], []
    stride = 4 * radix
    for high in range(radix):
        held = []
        for i in range(2):
            held.append(tuple(x[pl.ds(high * 4 + i * 2 + c, rows_hi, stride=stride), :] for c in range(2)))
        helds.append((held, [tuple(roll(v, half) for v in pair) for pair in held]))
        stage.append([])

    def advance(o):
        for high in range(radix):
            held, turned = helds[high]
            total = None
            for i in range(2):
                total = add(total, complex_mul(same[o][i], held[i]))
                total = add(total, complex_mul(cross[o][i], turned[i]))
            stage[high].append(total)

    advance(0)
    sign = jnp.where(field % 2 == 0, -1.0, 1.0)
    mixers = [[entry(split_gate, take, f) for f in range(radix)] for take in range(radix)]
    mixers = [[(re, im * sign) for re, im in line] for line in mixers]

    def merged(out_high, which):
        coefs = [entry(high_gate, out_high, high) for high in range(radix)]
        held = []
        for o in which:
            total = None
            for high in range(radix):
                total = add(total, complex_mul(coefs[high], stage[high][o]))
            held.append(total)
        return held

    def transposed(held):
        turned = {}
        for o in range(2):
            for c in range(2):
                for d in range(2 * o - 3, 2 * o + 2):
                    turned[o, c, d] = roll(held[o][c], d * group)
        blocks = []
        for f in range(radix):
            pair = []
            for flip in range(2):
                block = None
                for o in range(2):
                    for c in range(2):
                        piece = turned[o, c ^ flip, 2 * o + c - f]
                        block = piece if block is None else jnp.where(field == 2 * o + c, piece, block)
                pair.append(block)
            blocks.append(pair)
        return blocks

    def put_main(out_high, held, take):
        real, imag = held[take // 2]
        if take % 2:
            main = jnp.where(first, roll(real, half), imag)
        else:
            main = jnp.where(first, real, roll(imag, half))
        send[out_high * radix + take, :rows_hi] = main

    def put_extra(out_high, blocks, take):
        block = None
        for f in range(radix):
            re, im = mixers[take][f]
            term = re * blocks[f][0] + im * blocks[f][1]
            block = term if block is None else block + term
        own = (take % 2) * 2 + take // 2
        moved = [roll(block[rows_hi - tail :], 2 * group * (own - k)) for k in range(radix) if k != own]
        send[out_high * radix + take, rows_hi:] = jnp.where(
            outer[: rows_hi - tail] == own, jnp.concatenate(moved, axis=0), block[: rows_hi - tail]
        )

    def post(seat, level, rows):
        pltpu.make_async_remote_copy(
            src_ref=send.at[seat * radix + level, rows],
            dst_ref=recv.at[me, rows],
            send_sem=send_sem,
            recv_sem=recv_sem.at[n],
            device_id={"wide": seat, "narrow": level},
            device_id_type=MESH,
        ).start()

    def lowest(first_seat, rows):
        last_seat = first_seat + 1
        alone = (n == 0) & (lax.div(w, 2) == first_seat // 2)
        other_seat = first_seat + last_seat - w

        def body(seat, carry):
            post(seat, 0, rows)
            return carry

        lax.fori_loop(
            jnp.where(alone, other_seat, first_seat), jnp.where(alone, other_seat, last_seat) + 1, body, 0
        )

    whole = pl.ds(0, rows_all)

    def below(level, carry):
        for seat in seats:
            post(seat, level, whole)
        return carry

    def above(level, carry):
        for side, pair in ((row, seats[2:]), (1 - row, seats[:2])):
            pl.semaphore_wait(known.at[level, side], 2)
            for seat in pair:
                post(seat, level, whole)
        return carry

    early, opened = {}, {}
    for out_high in range(2):
        early[out_high] = merged(out_high, (0,))
        put_main(out_high, early[out_high], 0)

    def meet():
        @pl.when(core == 0)
        def _():
            pl.semaphore_wait(known.at[n, row], 1)

        @pl.when(row == 0)
        def _():
            pl.semaphore_wait(known.at[n, 1], 2)


    @pl.when(n == 0)
    def _():
        meet()

    lowest(0, pl.ds(0, rows_hi))
    advance(1)
    for out_high in range(2):
        early[out_high] += merged(out_high, (1,))
        opened[out_high] = transposed(early[out_high])
        put_extra(out_high, opened[out_high], 0)

    lowest(0, pl.ds(rows_hi, rows_all - rows_hi))

    for out_high in (2, 3, 0, 1):
        if out_high in early:
            held, blocks = early[out_high], opened[out_high]
        else:
            held = merged(out_high, (0, 1))
            blocks = transposed(held)
        for take in range(1 if out_high in early else 0, radix):
            put_main(out_high, held, take)
            put_extra(out_high, blocks, take)

    def own_level():
        meet()
        for seat in seats[:-1]:
            post(seat, n, whole)

    lowest(2, whole)

    @pl.when(n == 2)
    def _():
        own_level()
        above(3, 0)

    lax.fori_loop(1, n, below, 0)

    @pl.when((n == 1) | (n == 3))
    def _():
        own_level()

    lax.fori_loop(jnp.where(n == 2, radix, n + 1), radix, above, 0)
    recv[me] = send[w * radix + n]

    for begin in range(slots, total_pairs, slots):
        gate.update(merge(order[begin : begin + slots]))
    low = kron_all([gate[pair] for pair in range(start - 2, -1, -1)])
    block = jnp.concatenate(
        [jnp.concatenate([low[0], low[1]], axis=1), jnp.concatenate([-low[1], low[0]], axis=1)], axis=0
    )
    block = jnp.concatenate([jnp.concatenate([block] * radix, axis=0)] * radix, axis=1)
    down = lax.broadcasted_iota(jnp.int32, (LANES, LANES), 0)
    across = lax.broadcasted_iota(jnp.int32, (LANES, LANES), 1)
    grouped = jnp.where(down // (2 * group) == across // (2 * group), block, 0.0).T
    parts = kron_all([gate[pair] for pair in range(start - 1, -1, -1)])
    plain = jnp.concatenate(
        [jnp.concatenate([parts[0], parts[1]], axis=1), jnp.concatenate([-parts[1], parts[0]], axis=1)],
        axis=0,
    ).T
    stripes = range(0, LANES, 2 * group)
    grouped = jnp.concatenate(
        [grouped[at + shift : at + shift + group] for shift in (0, group) for at in stripes], axis=0
    )
    for index, item in enumerate((plain, grouped)):
        lane_hi[index], lane_lo[index] = split(item)
    row_members = [gate[pair] for pair in range(total_pairs - 1, start + 1, -1)]
    real, imag = (split(item) for item in kron_all(row_members))
    for at, into in enumerate((row_hi, row_lo)):
        for source in range(count):
            seat, level = source // radix, source % radix
            rows = slice(source * rows_hi, (source + 1) * rows_hi)
            place = slice(seat * rows_hi, (seat + 1) * rows_hi)
            into[0, level, place] = jnp.concatenate([real[at][rows], imag[at][rows]], axis=1)
            into[1, level, place] = jnp.concatenate([-imag[at][rows], real[at][rows]], axis=1)

    def settled(group, size):
        return pltpu.make_async_remote_copy(
            src_ref=send.at[pl.ds(0, size)],
            dst_ref=recv.at[pl.ds(0, size)],
            send_sem=send_sem,
            recv_sem=recv_sem.at[group],
            device_id={"wide": w, "narrow": n},
            device_id_type=MESH,
        )

    near, far = pairs_of(n)
    settled(near[0], radix - 1).wait_recv()
    settled(near[1], radix).wait_recv()
    acc[...] = contribution(radix, recv, (lane_hi, lane_lo), (row_hi, row_lo), near, n)
    settled(0, count - 1).wait_send()
    for level in far:
        settled(level, radix).wait_recv()


def finish_kernel(radix, recv, acc, lane_hi, lane_lo, row_hi, row_lo, out_hbm, marg_hbm, fin, prob, marg, sems):
    half = LANES // 2
    group = half // radix
    size = acc.shape[1] // 2
    blocks = size // LANES
    n = lax.axis_index("narrow")
    own = (n % 2) * 2 + n // 2
    total = acc[...] + contribution(radix, recv, (lane_hi, lane_lo), (row_hi, row_lo), pairs_of(n)[1], n)
    real, imag = total[:, :size], total[:, size:]
    for block in range(blocks):
        columns = slice(block * LANES, (block + 1) * LANES)
        fin[pl.ds(block * 2, half, stride=2 * blocks), :] = real[:half, columns]
        fin[pl.ds(block * 2 + 1, half, stride=2 * blocks), :] = imag[:half, columns]
    out_copy = pltpu.make_async_copy(fin, out_hbm, sems.at[0])
    out_copy.start()
    density = real * real + imag * imag
    for index in range(radix):
        prob[index] = density[index * group : (index + 1) * group]
    total = prob[n]
    for index in range(radix):
        at = half + group * index
        total = total + jnp.where(own == index, 0.0, density[at : at + group])
    for block in range(blocks):
        marg[pl.ds(block, group, stride=blocks), :] = total[:, block * LANES : (block + 1) * LANES]
    marg_copy = pltpu.make_async_copy(marg, marg_hbm, sems.at[1])
    marg_copy.start()
    out_copy.wait()
    marg_copy.wait()


def window_plan(wide_count, narrow_count, amplitudes, gates_shape):
    layers, pairs, radix = gates_shape[0], gates_shape[1], gates_shape[-1]
    high_bits = (wide_count * narrow_count).bit_length() - 1
    local_bits = amplitudes.bit_length() - 1
    total_bits = high_bits + local_bits
    if high_bits % 2 or local_bits % 2 or wide_count != radix or narrow_count != radix:
        return None
    if 2 * pairs != local_bits:
        return None
    offset = ((layers - 1) * high_bits) % total_bits
    start = offset // 2 - high_bits // 2
    if layers & (layers - 1) or LANES % (layers * radix) or start < 2 or LANES < 3 * layers * radix or offset // 2 >= pairs or 2 * radix**start != LANES:
        return None
    rows_hi = radix ** (pairs - offset // 2)
    if rows_hi % 8:
        return None
    for which in range(total_bits // 2):
        if all((which - layer * (high_bits // 2)) % (total_bits // 2) >= pairs for layer in range(layers)):
            return None
    return (layers, pairs, high_bits // 2, total_bits // 2, start, radix), rows_hi


def merged_local(plan, rows_hi, state, gates):
    radix = plan[-1]
    amplitudes = state.shape[-1]
    rows = amplitudes // LANES
    count = radix * radix
    own = amplitudes // radix // LANES
    x = jnp.swapaxes(state.reshape(2, rows, LANES), 0, 1).reshape(2 * rows, LANES)
    g = jnp.transpose(gates, (1, 2, 3, 4, 0)).reshape(-1, radix, gates.shape[0])
    f32, bf16 = jnp.float32, jnp.bfloat16
    size = count * rows_hi
    message = 2 * rows_hi - rows_hi // radix
    shared = (
        pltpu.VMEM((count, message, LANES), f32),
        pltpu.VMEM((LANES, 2 * size), f32),
        pltpu.VMEM((2, LANES, LANES), bf16),
        pltpu.VMEM((2, LANES, LANES), bf16),
        pltpu.VMEM((2, radix, size // radix, 2 * size), bf16),
        pltpu.VMEM((2, radix, size // radix, 2 * size), bf16),
    )
    held = pl.pallas_call(
        functools.partial(exchange_kernel, plan),
        out_shape=shared,
        in_specs=[pl.BlockSpec(memory_space=pltpu.HBM)] * 2,
        out_specs=[pl.BlockSpec(memory_space=pltpu.VMEM)] * len(shared),
        scratch_shapes=[
            pltpu.VMEM(x.shape, f32),
            pltpu.VMEM(g.shape, f32),
            pltpu.VMEM((count, message, LANES), f32),
            pltpu.SemaphoreType.DMA((2,)),
            pltpu.SemaphoreType.DMA,
            pltpu.SemaphoreType.DMA((radix,)),
            pltpu.SemaphoreType.REGULAR((radix, 2)),
        ],
        compiler_params=pltpu.CompilerParams(
            collective_id=0, has_side_effects=True, vmem_limit_bytes=8 * 2**20
        ),
        name="exchange",
    )(
        pltpu.with_memory_space_constraint(x, pltpu.HBM),
        pltpu.with_memory_space_constraint(g, pltpu.HBM),
    )
    out, marg = pl.pallas_call(
        functools.partial(finish_kernel, radix),
        out_shape=(pltpu.HBM((2 * rows, LANES), f32), pltpu.HBM((own, LANES), f32)),
        in_specs=[pl.BlockSpec(memory_space=pltpu.VMEM)] * len(shared),
        out_specs=[pl.BlockSpec(memory_space=pltpu.HBM)] * 2,
        scratch_shapes=[
            pltpu.VMEM((2 * rows, LANES), f32),
            pltpu.VMEM((radix, LANES // 2 // radix, size), f32),
            pltpu.VMEM((own, LANES), f32),
            pltpu.SemaphoreType.DMA((2,)),
        ],
        compiler_params=pltpu.CompilerParams(vmem_limit_bytes=8 * 2**20),
        name="finish",
    )(*held)
    final = jnp.swapaxes(out.reshape(rows, 2, LANES), 0, 1).reshape(1, 1, 2, amplitudes)
    return final, marg.reshape(1, -1)


def local(state, gates):
    wide_count = lax.axis_size("wide")
    narrow_count = lax.axis_size("narrow")
    amplitudes = state.shape[-1]
    found = window_plan(wide_count, narrow_count, amplitudes, gates.shape)
    if found is not None:
        return merged_local(*found, state, gates)
    flat = state.reshape(2, amplitudes)
    for layer_index in range(gates.shape[0]):
        if layer_index > 0:
            flat = rotate(flat, wide_count, narrow_count)
        flat = apply_layer(flat, gates[layer_index])
    prob = flat[0] * flat[0] + flat[1] * flat[1]
    marginal = lax.psum_scatter(prob, "narrow", scatter_dimension=0, tiled=True)
    return (flat.reshape(1, 1, 2, amplitudes), marginal.reshape(1, -1))


def solution(mesh):
    in_specs = (P(("slices", "wide"), "narrow", None, None), P())
    out_specs = (P(("slices", "wide"), "narrow", None, None), P(("slices", "wide"), "narrow"))
    return jax.shard_map(local, mesh=mesh, in_specs=in_specs, out_specs=out_specs, check_vma=False)
```

```python
import functools

import jax
import jax.numpy as jnp
from jax import lax
from jax.experimental import pallas as pl
from jax.experimental.pallas import tpu as pltpu
from jax.sharding import PartitionSpec as P


def kron_chain(members):
    real_part = members[0][0]
    imag_part = members[0][1]
    for member in members[1:]:
        other_real = member[0]
        other_imag = member[1]
        new_real = jnp.kron(real_part, other_real) - jnp.kron(imag_part, other_imag)
        new_imag = jnp.kron(real_part, other_imag) + jnp.kron(imag_part, other_real)
        real_part, imag_part = (new_real, new_imag)
    return (real_part, imag_part)


def rotate(flat, wide_count, narrow_count):
    devices = wide_count * narrow_count
    amplitudes = flat.shape[1]
    rest = amplitudes // devices
    blocks = flat.reshape(2, rest, devices)
    turned = jnp.swapaxes(blocks, 1, 2)
    moved = lax.all_to_all(turned, ("wide", "narrow"), split_axis=1, concat_axis=1, tiled=True)
    return moved.reshape(2, amplitudes)


def apply_layer(flat, layer_gates):
    amplitudes = flat.shape[1]
    pairs = layer_gates.shape[0]
    upper = amplitudes // 256
    low_real, low_imag = kron_chain([layer_gates[index] for index in range(3, -1, -1)])
    high_real, high_imag = kron_chain([layer_gates[index] for index in range(pairs - 1, 3, -1)])
    blocks = flat.reshape(2, upper, 256)
    real_rows = blocks[0]
    imag_rows = blocks[1]
    highest = lax.Precision.HIGHEST
    next_real = jnp.dot(real_rows, low_real.T, precision=highest) - jnp.dot(
        imag_rows, low_imag.T, precision=highest
    )
    next_imag = jnp.dot(real_rows, low_imag.T, precision=highest) + jnp.dot(
        imag_rows, low_real.T, precision=highest
    )
    final_real = jnp.dot(high_real, next_real, precision=highest) - jnp.dot(
        high_imag, next_imag, precision=highest
    )
    final_imag = jnp.dot(high_imag, next_real, precision=highest) + jnp.dot(
        high_real, next_imag, precision=highest
    )
    return jnp.stack([final_real, final_imag]).reshape(2, amplitudes)


MESH = pl.DeviceIdType.MESH
LANES = 128


def complex_mul(left, right):
    return (
        left[0] * right[0] - left[1] * right[1],
        left[0] * right[1] + left[1] * right[0],
    )


def take_lanes(value, source):
    return jnp.take_along_axis(value, source, axis=1, mode="promise_in_bounds")


def gate_tools(g, plan):
    layers, pairs, shift, total_pairs, _, radix = plan
    shape = (2 * radix, LANES)
    lane = lax.broadcasted_iota(jnp.int32, shape, 1)
    down = lax.broadcasted_iota(jnp.int32, shape, 0)
    width = radix * layers
    layer, row, slot = lane % layers, (lane // layers) % radix, lane // width
    pad = jnp.zeros((radix, LANES - layers), jnp.float32)
    tiles, planes = [], []
    for pair in range(pairs):
        tiles.append([])
        plane = None
        for at in range(radix):
            tile = jnp.concatenate(
                [jnp.concatenate([g[(pair * 2 + c) * radix + at], pad], axis=1) for c in range(2)], axis=0
            )
            tiles[-1].append(tile)
            tile = take_lanes(tile, layer)
            plane = tile if plane is None else jnp.where(row == at, tile, plane)
        planes.append(plane)
    sign = jnp.where(down < radix, -1.0, 1.0)

    def merge(held, direct=False):
        place = held[0] - shift * layer
        for index, pair in enumerate(held[1:]):
            place = jnp.where(slot == index + 1, pair - shift * layer, place)
        for _ in range(-(-layers * shift // total_pairs)):
            place = jnp.where(place < 0, place + total_pairs, place)
        total = jnp.where(down == row, 1.0, 0.0)
        for pair in range(pairs):
            total = jnp.where(place == pair, planes[pair], total)
        step = 1
        while step < layers:
            before = jnp.maximum(layer - step, 0)
            straight, crossed = None, None
            for at in range(radix):
                if direct and step == 1:
                    early = jnp.where(down == at, 1.0, 0.0)
                    previous = jnp.where(place + shift < total_pairs, place + shift, place + shift - total_pairs)
                    for pair in range(pairs):
                        early = jnp.where(previous == pair, take_lanes(tiles[pair][at], before), early)
                else:
                    early = take_lanes(total, slot * width + at * layers + before)
                one_part = total[at : at + 1] * early
                two_part = total[radix + at : radix + at + 1] * early
                straight = one_part if straight is None else straight + one_part
                crossed = two_part if crossed is None else crossed + two_part
            total = straight + sign * pltpu.roll(crossed, radix, 0)
            step *= 2
        return {
            pair: [
                take_lanes(total, jnp.full(shape, index * width + (at + 1) * layers - 1, jnp.int32))
                for at in range(radix)
            ]
            for index, pair in enumerate(held)
        }

    return merge


def kron_all(members):
    radix = len(members[0])
    size = radix ** len(members)
    width = max(size, LANES)
    lane = lax.broadcasted_iota(jnp.int32, (2 * radix, width), 1)
    rows = None
    for place, member in enumerate(reversed(members)):
        field = (lane // radix**place) % radix
        columns = [jnp.concatenate([column] * (width // LANES), axis=1) for column in member]
        spread = columns[-1]
        for index in range(radix - 1):
            spread = jnp.where(field == index, columns[index], spread)
        wide = spread[:radix], spread[radix:]
        if rows is None:
            rows = wide
            continue
        pieces = [
            complex_mul(tuple(part[index : index + 1, :] for part in wide), rows)
            for index in range(radix)
        ]
        rows = tuple(jnp.concatenate([piece[c] for piece in pieces], axis=0) for c in range(2))
    return tuple(part[:, :size] for part in rows)


def split(value):
    high = value.astype(jnp.bfloat16)
    return high, (value - high.astype(jnp.float32)).astype(jnp.bfloat16)


def precise(left, right, contract):
    def one(a, b):
        return lax.dot_general(a, b, (((1,), (contract,)), ((), ())), preferred_element_type=jnp.float32)

    return one(left[0], right[0]) + (one(left[0], right[1]) + one(left[1], right[0]))


def precise_one(a, b):
    return lax.dot_general(a, b, (((1,), (0,)), ((), ())), preferred_element_type=jnp.float32)


def pairs_of(n):
    near = n, jnp.where(n == 0, 1, n - 1)
    return near, (jnp.where(n < 2, 2, 0), jnp.where(n < 3, 3, 1))


def contribution(radix, recv, lanes, rows, levels, n):
    held = jnp.concatenate([recv[pl.ds(level * radix, radix)] for level in levels], axis=0)
    rows_hi = held.shape[1] * radix // (2 * radix - 1)
    tail = rows_hi // radix
    size = held.shape[0] * rows_hi
    wide = LANES // radix
    packed = held[:, rows_hi:]
    outer = lax.broadcasted_iota(jnp.int32, (1, tail, LANES), 2) // wide
    own = (n % 2) * 2 + n // 2
    last = packed[:, :tail]
    for index in range(radix - 1):
        kept = index + jnp.where(own <= index, 1, 0)
        piece = packed[:, index * tail : (index + 1) * tail]
        piece = pltpu.roll(piece, lax.rem(wide * (kept - own) + LANES, LANES), 2)
        last = jnp.where(outer == kept, piece, last)
    turned = []
    for which, value in enumerate((held[:, :rows_hi], jnp.concatenate([packed, last], axis=1))):
        item = precise(tuple(part[which] for part in lanes), split(value.reshape(size, LANES)), 1)
        turned.append(jnp.concatenate([item[: LANES // 2], item[LANES // 2 :]], axis=1))
    matrix = [
        jnp.concatenate([part[c, level] for c in range(2) for level in levels], axis=0) for part in rows
    ]
    high, low = split(jnp.concatenate(turned, axis=0))
    both = precise_one(jnp.concatenate([high, low], axis=0), matrix[0])
    rows = high.shape[0]
    return both[:rows] + (both[rows:] + precise_one(high, matrix[1]))


def greet(semaphore, seat, level):
    pl.semaphore_signal(semaphore, inc=1, device_id={"wide": seat, "narrow": level}, device_id_type=MESH)


def exchange_kernel(plan, x_hbm, g_hbm, recv, acc, lane_hi, lane_lo, row_hi, row_lo, x, g, send,
                    local_sem, send_sem, recv_sem, known):
    layers, pairs, shift, total_pairs, start, radix = plan
    w = lax.axis_index("wide")
    n = lax.axis_index("narrow")
    me = n * radix + w
    count = radix * radix

    barrier = pltpu.get_barrier_semaphore()
    copy_g = pltpu.make_async_copy(g_hbm, g, local_sem.at[0])
    copy_x = pltpu.make_async_copy(x_hbm, x, local_sem.at[1])
    copy_g.start()
    copy_x.start()
    row, core = lax.div(w, 2), lax.rem(w, 2)
    other = 2 * (1 - row)
    ordered = [other + 1, other, 2 * row + 1, 2 * row]
    seats = [other + core, other + 1 - core, 2 * row + 1 - core, w]
    for seat in range(1, radix):
        @pl.when(seat > w)
        def _():
            greet(barrier, seat, n)

    for level in range(1, radix):
        @pl.when(level > n)
        def _():
            for seat in range(radix):
                greet(barrier, seat, level)

    @pl.when(me > 0)
    def _():
        pl.semaphore_wait(barrier, me)

    for level in range(radix - 2, -1, -1):
        @pl.when(level < n)
        def _():
            for seat in range(radix):
                greet(known.at[n, row], seat, level)

    for seat in range(radix - 1):
        @pl.when(seat < w)
        def _():
            greet(known.at[n, row], seat, n)

    copy_g.wait()
    copy_x.wait()

    merge = gate_tools(g, plan)
    order = list(range(start - 1, start + 2)) + list(range(start - 1)) + list(range(start + 2, total_pairs))
    slots = LANES // (radix * layers)
    gate = merge(order[:slots], True)
    split_gate, low_gate, high_gate = (gate[pair] for pair in range(start - 1, start + 2))

    half = LANES // 2
    group = half // radix
    rows_all = send.shape[1]
    rows_hi = rows_all * radix // (2 * radix - 1)
    tail = rows_hi // radix
    shape = (rows_hi, LANES)
    lane = lax.broadcasted_iota(jnp.int32, shape, 1)
    first = lane < half
    field = (lane // group) % radix
    outer = lane // (2 * group)

    def entry(gate, row, column):
        return tuple(
            jnp.broadcast_to(gate[row][at : at + 1], shape) for at in (column, column + radix)
        )

    def both(gate, one, other):
        return tuple(jnp.where(first, a, b) for a, b in zip(entry(gate, *one), entry(gate, *other)))

    def add(total, term):
        return term if total is None else (total[0] + term[0], total[1] + term[1])

    def roll(value, amount):
        amount %= LANES
        return pltpu.roll(value, amount, 1) if amount else value

    same = [[both(low_gate, (2 * o, 2 * i), (2 * o + 1, 2 * i + 1)) for i in range(2)] for o in range(2)]
    cross = [[both(low_gate, (2 * o, 2 * i + 1), (2 * o + 1, 2 * i)) for i in range(2)] for o in range(2)]
    helds, stage = [], []
    stride = 4 * radix
    for high in range(radix):
        held = []
        for i in range(2):
            held.append(tuple(x[pl.ds(high * 4 + i * 2 + c, rows_hi, stride=stride), :] for c in range(2)))
        helds.append((held, [tuple(roll(v, half) for v in pair) for pair in held]))
        stage.append([])

    def advance(o):
        for high in range(radix):
            held, turned = helds[high]
            total = None
            for i in range(2):
                total = add(total, complex_mul(same[o][i], held[i]))
                total = add(total, complex_mul(cross[o][i], turned[i]))
            stage[high].append(total)

    advance(0)
    sign = jnp.where(field % 2 == 0, -1.0, 1.0)
    mixers = [[entry(split_gate, take, f) for f in range(radix)] for take in range(radix)]
    mixers = [[(re, im * sign) for re, im in line] for line in mixers]

    def merged(out_high, which):
        coefs = [entry(high_gate, out_high, high) for high in range(radix)]
        held = []
        for o in which:
            total = None
            for high in range(radix):
                total = add(total, complex_mul(coefs[high], stage[high][o]))
            held.append(total)
        return held

    def transposed(held):
        turned = {}
        for o in range(2):
            for c in range(2):
                for d in range(2 * o - 3, 2 * o + 2):
                    turned[o, c, d] = roll(held[o][c], d * group)
        blocks = []
        for f in range(radix):
            pair = []
            for flip in range(2):
                block = None
                for o in range(2):
                    for c in range(2):
                        piece = turned[o, c ^ flip, 2 * o + c - f]
                        block = piece if block is None else jnp.where(field == 2 * o + c, piece, block)
                pair.append(block)
            blocks.append(pair)
        return blocks

    def put_main(out_high, held, take):
        real, imag = held[take // 2]
        if take % 2:
            main = jnp.where(first, roll(real, half), imag)
        else:
            main = jnp.where(first, real, roll(imag, half))
        send[out_high * radix + take, :rows_hi] = main

    def put_extra(out_high, blocks, take):
        block = None
        for f in range(radix):
            re, im = mixers[take][f]
            term = re * blocks[f][0] + im * blocks[f][1]
            block = term if block is None else block + term
        own = (take % 2) * 2 + take // 2
        moved = [roll(block[rows_hi - tail :], 2 * group * (own - k)) for k in range(radix) if k != own]
        send[out_high * radix + take, rows_hi:] = jnp.where(
            outer[: rows_hi - tail] == own, jnp.concatenate(moved, axis=0), block[: rows_hi - tail]
        )

    def post(seat, level, rows):
        pltpu.make_async_remote_copy(
            src_ref=send.at[seat * radix + level, rows],
            dst_ref=recv.at[me, rows],
            send_sem=send_sem,
            recv_sem=recv_sem.at[n],
            device_id={"wide": seat, "narrow": level},
            device_id_type=MESH,
        ).start()

    def lowest(first_seat, rows):
        last_seat = first_seat + 1
        alone = (n == 0) & (lax.div(w, 2) == first_seat // 2)
        other_seat = first_seat + last_seat - w

        def body(seat, carry):
            post(seat, 0, rows)
            return carry

        lax.fori_loop(
            jnp.where(alone, other_seat, first_seat), jnp.where(alone, other_seat, last_seat) + 1, body, 0
        )

    whole = pl.ds(0, rows_all)

    def below(level, carry):
        for seat in seats:
            post(seat, level, whole)
        return carry

    def above(level, carry):
        for side, pair in ((row, ordered[2:]), (1 - row, ordered[:2])):
            pl.semaphore_wait(known.at[level, side], 2)
            for seat in pair:
                post(seat, level, whole)
        return carry

    early, opened = {}, {}
    for out_high in range(2):
        early[out_high] = merged(out_high, (0,))
        put_main(out_high, early[out_high], 0)

    def meet():
        @pl.when(core == 0)
        def _():
            pl.semaphore_wait(known.at[n, row], 1)

        @pl.when(row == 0)
        def _():
            pl.semaphore_wait(known.at[n, 1], 2)


    @pl.when(n == 0)
    def _():
        meet()

    lowest(0, pl.ds(0, rows_hi))
    advance(1)
    for out_high in range(2):
        early[out_high] += merged(out_high, (1,))
        opened[out_high] = transposed(early[out_high])
        put_extra(out_high, opened[out_high], 0)

    lowest(0, pl.ds(rows_hi, rows_all - rows_hi))

    for out_high in (2, 3, 0, 1):
        if out_high in early:
            held, blocks = early[out_high], opened[out_high]
        else:
            held = merged(out_high, (0, 1))
            blocks = transposed(held)
        for take in range(1 if out_high in early else 0, radix):
            put_main(out_high, held, take)
            put_extra(out_high, blocks, take)

    def own_level():
        meet()
        for seat in seats[:-1]:
            post(seat, n, whole)

    lowest(2, whole)

    @pl.when(n == 2)
    def _():
        own_level()
        above(3, 0)

    lax.fori_loop(1, n, below, 0)

    @pl.when((n == 1) | (n == 3))
    def _():
        own_level()

    lax.fori_loop(jnp.where(n == 2, radix, n + 1), radix, above, 0)
    recv[me] = send[w * radix + n]

    for begin in range(slots, total_pairs, slots):
        gate.update(merge(order[begin : begin + slots]))
    low = kron_all([gate[pair] for pair in range(start - 2, -1, -1)])
    block = jnp.concatenate(
        [jnp.concatenate([low[0], low[1]], axis=1), jnp.concatenate([-low[1], low[0]], axis=1)], axis=0
    )
    block = jnp.concatenate([jnp.concatenate([block] * radix, axis=0)] * radix, axis=1)
    down = lax.broadcasted_iota(jnp.int32, (LANES, LANES), 0)
    across = lax.broadcasted_iota(jnp.int32, (LANES, LANES), 1)
    grouped = jnp.where(down // (2 * group) == across // (2 * group), block, 0.0).T
    parts = kron_all([gate[pair] for pair in range(start - 1, -1, -1)])
    plain = jnp.concatenate(
        [jnp.concatenate([parts[0], parts[1]], axis=1), jnp.concatenate([-parts[1], parts[0]], axis=1)],
        axis=0,
    ).T
    stripes = range(0, LANES, 2 * group)
    grouped = jnp.concatenate(
        [grouped[at + shift : at + shift + group] for shift in (0, group) for at in stripes], axis=0
    )
    for index, item in enumerate((plain, grouped)):
        lane_hi[index], lane_lo[index] = split(item)
    row_members = [gate[pair] for pair in range(total_pairs - 1, start + 1, -1)]
    real, imag = (split(item) for item in kron_all(row_members))
    for at, into in enumerate((row_hi, row_lo)):
        for source in range(count):
            seat, level = source // radix, source % radix
            rows = slice(source * rows_hi, (source + 1) * rows_hi)
            place = slice(seat * rows_hi, (seat + 1) * rows_hi)
            into[0, level, place] = jnp.concatenate([real[at][rows], imag[at][rows]], axis=1)
            into[1, level, place] = jnp.concatenate([-imag[at][rows], real[at][rows]], axis=1)

    def settled(group, size):
        return pltpu.make_async_remote_copy(
            src_ref=send.at[pl.ds(0, size)],
            dst_ref=recv.at[pl.ds(0, size)],
            send_sem=send_sem,
            recv_sem=recv_sem.at[group],
            device_id={"wide": w, "narrow": n},
            device_id_type=MESH,
        )

    near, far = pairs_of(n)
    settled(near[0], radix - 1).wait_recv()
    settled(near[1], radix).wait_recv()
    acc[...] = contribution(radix, recv, (lane_hi, lane_lo), (row_hi, row_lo), near, n)
    settled(0, count - 1).wait_send()
    for level in far:
        settled(level, radix).wait_recv()


def finish_kernel(radix, recv, acc, lane_hi, lane_lo, row_hi, row_lo, out_hbm, marg_hbm, fin, prob, marg, sems):
    half = LANES // 2
    group = half // radix
    size = acc.shape[1] // 2
    blocks = size // LANES
    n = lax.axis_index("narrow")
    own = (n % 2) * 2 + n // 2
    total = acc[...] + contribution(radix, recv, (lane_hi, lane_lo), (row_hi, row_lo), pairs_of(n)[1], n)
    real, imag = total[:, :size], total[:, size:]
    for block in range(blocks):
        columns = slice(block * LANES, (block + 1) * LANES)
        fin[pl.ds(block * 2, half, stride=2 * blocks), :] = real[:half, columns]
        fin[pl.ds(block * 2 + 1, half, stride=2 * blocks), :] = imag[:half, columns]
    out_copy = pltpu.make_async_copy(fin, out_hbm, sems.at[0])
    out_copy.start()
    density = real * real + imag * imag
    for index in range(radix):
        prob[index] = density[index * group : (index + 1) * group]
    total = prob[n]
    for index in range(radix):
        at = half + group * index
        total = total + jnp.where(own == index, 0.0, density[at : at + group])
    for block in range(blocks):
        marg[pl.ds(block, group, stride=blocks), :] = total[:, block * LANES : (block + 1) * LANES]
    marg_copy = pltpu.make_async_copy(marg, marg_hbm, sems.at[1])
    marg_copy.start()
    out_copy.wait()
    marg_copy.wait()


def window_plan(wide_count, narrow_count, amplitudes, gates_shape):
    layers, pairs, radix = gates_shape[0], gates_shape[1], gates_shape[-1]
    high_bits = (wide_count * narrow_count).bit_length() - 1
    local_bits = amplitudes.bit_length() - 1
    total_bits = high_bits + local_bits
    if high_bits % 2 or local_bits % 2 or wide_count != radix or narrow_count != radix:
        return None
    if 2 * pairs != local_bits:
        return None
    offset = ((layers - 1) * high_bits) % total_bits
    start = offset // 2 - high_bits // 2
    if layers & (layers - 1) or LANES % (layers * radix) or start < 2 or LANES < 3 * layers * radix or offset // 2 >= pairs or 2 * radix**start != LANES:
        return None
    rows_hi = radix ** (pairs - offset // 2)
    if rows_hi % 8:
        return None
    for which in range(total_bits // 2):
        if all((which - layer * (high_bits // 2)) % (total_bits // 2) >= pairs for layer in range(layers)):
            return None
    return (layers, pairs, high_bits // 2, total_bits // 2, start, radix), rows_hi


def merged_local(plan, rows_hi, state, gates):
    radix = plan[-1]
    amplitudes = state.shape[-1]
    rows = amplitudes // LANES
    count = radix * radix
    own = amplitudes // radix // LANES
    x = jnp.swapaxes(state.reshape(2, rows, LANES), 0, 1).reshape(2 * rows, LANES)
    g = jnp.transpose(gates, (1, 2, 3, 4, 0)).reshape(-1, radix, gates.shape[0])
    f32, bf16 = jnp.float32, jnp.bfloat16
    size = count * rows_hi
    message = 2 * rows_hi - rows_hi // radix
    shared = (
        pltpu.VMEM((count, message, LANES), f32),
        pltpu.VMEM((LANES, 2 * size), f32),
        pltpu.VMEM((2, LANES, LANES), bf16),
        pltpu.VMEM((2, LANES, LANES), bf16),
        pltpu.VMEM((2, radix, size // radix, 2 * size), bf16),
        pltpu.VMEM((2, radix, size // radix, 2 * size), bf16),
    )
    held = pl.pallas_call(
        functools.partial(exchange_kernel, plan),
        out_shape=shared,
        in_specs=[pl.BlockSpec(memory_space=pltpu.HBM)] * 2,
        out_specs=[pl.BlockSpec(memory_space=pltpu.VMEM)] * len(shared),
        scratch_shapes=[
            pltpu.VMEM(x.shape, f32),
            pltpu.VMEM(g.shape, f32),
            pltpu.VMEM((count, message, LANES), f32),
            pltpu.SemaphoreType.DMA((2,)),
            pltpu.SemaphoreType.DMA,
            pltpu.SemaphoreType.DMA((radix,)),
            pltpu.SemaphoreType.REGULAR((radix, 2)),
        ],
        compiler_params=pltpu.CompilerParams(
            collective_id=0, has_side_effects=True, vmem_limit_bytes=8 * 2**20
        ),
        name="exchange",
    )(
        pltpu.with_memory_space_constraint(x, pltpu.HBM),
        pltpu.with_memory_space_constraint(g, pltpu.HBM),
    )
    out, marg = pl.pallas_call(
        functools.partial(finish_kernel, radix),
        out_shape=(pltpu.HBM((2 * rows, LANES), f32), pltpu.HBM((own, LANES), f32)),
        in_specs=[pl.BlockSpec(memory_space=pltpu.VMEM)] * len(shared),
        out_specs=[pl.BlockSpec(memory_space=pltpu.HBM)] * 2,
        scratch_shapes=[
            pltpu.VMEM((2 * rows, LANES), f32),
            pltpu.VMEM((radix, LANES // 2 // radix, size), f32),
            pltpu.VMEM((own, LANES), f32),
            pltpu.SemaphoreType.DMA((2,)),
        ],
        compiler_params=pltpu.CompilerParams(vmem_limit_bytes=8 * 2**20),
        name="finish",
    )(*held)
    final = jnp.swapaxes(out.reshape(rows, 2, LANES), 0, 1).reshape(1, 1, 2, amplitudes)
    return final, marg.reshape(1, -1)


def local(state, gates):
    wide_count = lax.axis_size("wide")
    narrow_count = lax.axis_size("narrow")
    amplitudes = state.shape[-1]
    found = window_plan(wide_count, narrow_count, amplitudes, gates.shape)
    if found is not None:
        return merged_local(*found, state, gates)
    flat = state.reshape(2, amplitudes)
    for layer_index in range(gates.shape[0]):
        if layer_index > 0:
            flat = rotate(flat, wide_count, narrow_count)
        flat = apply_layer(flat, gates[layer_index])
    prob = flat[0] * flat[0] + flat[1] * flat[1]
    marginal = lax.psum_scatter(prob, "narrow", scatter_dimension=0, tiled=True)
    return (flat.reshape(1, 1, 2, amplitudes), marginal.reshape(1, -1))


def solution(mesh):
    in_specs = (P(("slices", "wide"), "narrow", None, None), P())
    out_specs = (P(("slices", "wide"), "narrow", None, None), P(("slices", "wide"), "narrow"))
    return jax.shard_map(local, mesh=mesh, in_specs=in_specs, out_specs=out_specs, check_vma=False)
```

```python
import functools

import jax
import jax.numpy as jnp
from jax import lax
from jax.experimental import pallas as pl
from jax.experimental.pallas import tpu as pltpu
from jax.sharding import PartitionSpec as P


def kron_chain(members):
    real_part = members[0][0]
    imag_part = members[0][1]
    for member in members[1:]:
        other_real = member[0]
        other_imag = member[1]
        new_real = jnp.kron(real_part, other_real) - jnp.kron(imag_part, other_imag)
        new_imag = jnp.kron(real_part, other_imag) + jnp.kron(imag_part, other_real)
        real_part, imag_part = (new_real, new_imag)
    return (real_part, imag_part)


def rotate(flat, wide_count, narrow_count):
    devices = wide_count * narrow_count
    amplitudes = flat.shape[1]
    rest = amplitudes // devices
    blocks = flat.reshape(2, rest, devices)
    turned = jnp.swapaxes(blocks, 1, 2)
    moved = lax.all_to_all(turned, ("wide", "narrow"), split_axis=1, concat_axis=1, tiled=True)
    return moved.reshape(2, amplitudes)


def apply_layer(flat, layer_gates):
    amplitudes = flat.shape[1]
    pairs = layer_gates.shape[0]
    upper = amplitudes // 256
    low_real, low_imag = kron_chain([layer_gates[index] for index in range(3, -1, -1)])
    high_real, high_imag = kron_chain([layer_gates[index] for index in range(pairs - 1, 3, -1)])
    blocks = flat.reshape(2, upper, 256)
    real_rows = blocks[0]
    imag_rows = blocks[1]
    highest = lax.Precision.HIGHEST
    next_real = jnp.dot(real_rows, low_real.T, precision=highest) - jnp.dot(
        imag_rows, low_imag.T, precision=highest
    )
    next_imag = jnp.dot(real_rows, low_imag.T, precision=highest) + jnp.dot(
        imag_rows, low_real.T, precision=highest
    )
    final_real = jnp.dot(high_real, next_real, precision=highest) - jnp.dot(
        high_imag, next_imag, precision=highest
    )
    final_imag = jnp.dot(high_imag, next_real, precision=highest) + jnp.dot(
        high_real, next_imag, precision=highest
    )
    return jnp.stack([final_real, final_imag]).reshape(2, amplitudes)


MESH = pl.DeviceIdType.MESH
LANES = 128


def complex_mul(left, right):
    return (
        left[0] * right[0] - left[1] * right[1],
        left[0] * right[1] + left[1] * right[0],
    )


def take_lanes(value, source):
    return jnp.take_along_axis(value, source, axis=1, mode="promise_in_bounds")


def gate_tools(g, plan):
    layers, pairs, shift, total_pairs, _, radix = plan
    shape = (2 * radix, LANES)
    lane = lax.broadcasted_iota(jnp.int32, shape, 1)
    down = lax.broadcasted_iota(jnp.int32, shape, 0)
    width = radix * layers
    layer, row, slot = lane % layers, (lane // layers) % radix, lane // width
    pad = jnp.zeros((radix, LANES - layers), jnp.float32)
    tiles, planes = [], []
    for pair in range(pairs):
        tiles.append([])
        plane = None
        for at in range(radix):
            tile = jnp.concatenate(
                [jnp.concatenate([g[(pair * 2 + c) * radix + at], pad], axis=1) for c in range(2)], axis=0
            )
            tiles[-1].append(tile)
            tile = take_lanes(tile, layer)
            plane = tile if plane is None else jnp.where(row == at, tile, plane)
        planes.append(plane)
    sign = jnp.where(down < radix, -1.0, 1.0)

    def merge(held, direct=False):
        place = held[0] - shift * layer
        for index, pair in enumerate(held[1:]):
            place = jnp.where(slot == index + 1, pair - shift * layer, place)
        for _ in range(-(-layers * shift // total_pairs)):
            place = jnp.where(place < 0, place + total_pairs, place)
        total = jnp.where(down == row, 1.0, 0.0)
        for pair in range(pairs):
            total = jnp.where(place == pair, planes[pair], total)
        step = 1
        while step < layers:
            before = jnp.maximum(layer - step, 0)
            straight, crossed = None, None
            for at in range(radix):
                if direct and step == 1:
                    early = jnp.where(down == at, 1.0, 0.0)
                    previous = jnp.where(place + shift < total_pairs, place + shift, place + shift - total_pairs)
                    for pair in range(pairs):
                        early = jnp.where(previous == pair, take_lanes(tiles[pair][at], before), early)
                else:
                    early = take_lanes(total, slot * width + at * layers + before)
                one_part = total[at : at + 1] * early
                two_part = total[radix + at : radix + at + 1] * early
                straight = one_part if straight is None else straight + one_part
                crossed = two_part if crossed is None else crossed + two_part
            total = straight + sign * pltpu.roll(crossed, radix, 0)
            step *= 2
        return {
            pair: [
                take_lanes(total, jnp.full(shape, index * width + (at + 1) * layers - 1, jnp.int32))
                for at in range(radix)
            ]
            for index, pair in enumerate(held)
        }

    return merge


def kron_all(members):
    radix = len(members[0])
    size = radix ** len(members)
    width = max(size, LANES)
    lane = lax.broadcasted_iota(jnp.int32, (2 * radix, width), 1)
    rows = None
    for place, member in enumerate(reversed(members)):
        field = (lane // radix**place) % radix
        columns = [jnp.concatenate([column] * (width // LANES), axis=1) for column in member]
        spread = columns[-1]
        for index in range(radix - 1):
            spread = jnp.where(field == index, columns[index], spread)
        wide = spread[:radix], spread[radix:]
        if rows is None:
            rows = wide
            continue
        pieces = [
            complex_mul(tuple(part[index : index + 1, :] for part in wide), rows)
            for index in range(radix)
        ]
        rows = tuple(jnp.concatenate([piece[c] for piece in pieces], axis=0) for c in range(2))
    return tuple(part[:, :size] for part in rows)


def split(value):
    high = value.astype(jnp.bfloat16)
    return high, (value - high.astype(jnp.float32)).astype(jnp.bfloat16)


def precise(left, right, contract):
    def one(a, b):
        return lax.dot_general(a, b, (((1,), (contract,)), ((), ())), preferred_element_type=jnp.float32)

    return one(left[0], right[0]) + (one(left[0], right[1]) + one(left[1], right[0]))


def precise_one(a, b):
    return lax.dot_general(a, b, (((1,), (0,)), ((), ())), preferred_element_type=jnp.float32)


def pairs_of(n):
    near = n, jnp.where(n == 0, 1, n - 1)
    return near, (jnp.where(n < 2, 2, 0), jnp.where(n < 3, 3, 1))


def contribution(radix, recv, lanes, rows, levels, n):
    held = jnp.concatenate([recv[pl.ds(level * radix, radix)] for level in levels], axis=0)
    rows_hi = held.shape[1] * radix // (2 * radix - 1)
    tail = rows_hi // radix
    size = held.shape[0] * rows_hi
    wide = LANES // radix
    packed = held[:, rows_hi:]
    outer = lax.broadcasted_iota(jnp.int32, (1, tail, LANES), 2) // wide
    own = (n % 2) * 2 + n // 2
    last = packed[:, :tail]
    for index in range(radix - 1):
        kept = index + jnp.where(own <= index, 1, 0)
        piece = packed[:, index * tail : (index + 1) * tail]
        piece = pltpu.roll(piece, lax.rem(wide * (kept - own) + LANES, LANES), 2)
        last = jnp.where(outer == kept, piece, last)
    turned = []
    for which, value in enumerate((held[:, :rows_hi], jnp.concatenate([packed, last], axis=1))):
        item = precise(tuple(part[which] for part in lanes), split(value.reshape(size, LANES)), 1)
        turned.append(jnp.concatenate([item[: LANES // 2], item[LANES // 2 :]], axis=1))
    matrix = [
        jnp.concatenate([part[c, level] for c in range(2) for level in levels], axis=0) for part in rows
    ]
    high, low = split(jnp.concatenate(turned, axis=0))
    both = precise_one(jnp.concatenate([high, low], axis=0), matrix[0])
    rows = high.shape[0]
    return both[:rows] + (both[rows:] + precise_one(high, matrix[1]))


def greet(semaphore, seat, level):
    pl.semaphore_signal(semaphore, inc=1, device_id={"wide": seat, "narrow": level}, device_id_type=MESH)


def exchange_kernel(plan, x_hbm, g_hbm, recv, acc, lane_hi, lane_lo, row_hi, row_lo, x, g, send,
                    local_sem, send_sem, recv_sem, known):
    layers, pairs, shift, total_pairs, start, radix = plan
    w = lax.axis_index("wide")
    n = lax.axis_index("narrow")
    me = n * radix + w
    count = radix * radix

    barrier = pltpu.get_barrier_semaphore()
    copy_g = pltpu.make_async_copy(g_hbm, g, local_sem.at[0])
    copy_x = pltpu.make_async_copy(x_hbm, x, local_sem.at[1])
    copy_g.start()
    copy_x.start()
    row, core = lax.div(w, 2), lax.rem(w, 2)
    other = 2 * (1 - row)
    rows_first = [core, 1 - core, 2 + core, 3 - core]
    seats = [other + core, other + 1 - core, 2 * row + 1 - core, w]
    for seat in range(1, radix):
        @pl.when(seat > w)
        def _():
            greet(barrier, seat, n)

    for level in range(1, radix):
        @pl.when(level > n)
        def _():
            for seat in range(radix):
                greet(barrier, seat, level)

    @pl.when(me > 0)
    def _():
        pl.semaphore_wait(barrier, me)

    for level in range(radix - 2, -1, -1):
        @pl.when(level < n)
        def _():
            for seat in range(radix):
                greet(known.at[n, row], seat, level)

    for seat in range(radix - 1):
        @pl.when(seat < w)
        def _():
            greet(known.at[n, row], seat, n)

    copy_g.wait()
    copy_x.wait()

    merge = gate_tools(g, plan)
    order = list(range(start - 1, start + 2)) + list(range(start - 1)) + list(range(start + 2, total_pairs))
    slots = LANES // (radix * layers)
    gate = merge(order[:slots], True)
    split_gate, low_gate, high_gate = (gate[pair] for pair in range(start - 1, start + 2))

    half = LANES // 2
    group = half // radix
    rows_all = send.shape[1]
    rows_hi = rows_all * radix // (2 * radix - 1)
    tail = rows_hi // radix
    shape = (rows_hi, LANES)
    lane = lax.broadcasted_iota(jnp.int32, shape, 1)
    first = lane < half
    field = (lane // group) % radix
    outer = lane // (2 * group)

    def entry(gate, row, column):
        return tuple(
            jnp.broadcast_to(gate[row][at : at + 1], shape) for at in (column, column + radix)
        )

    def both(gate, one, other):
        return tuple(jnp.where(first, a, b) for a, b in zip(entry(gate, *one), entry(gate, *other)))

    def add(total, term):
        return term if total is None else (total[0] + term[0], total[1] + term[1])

    def roll(value, amount):
        amount %= LANES
        return pltpu.roll(value, amount, 1) if amount else value

    same = [[both(low_gate, (2 * o, 2 * i), (2 * o + 1, 2 * i + 1)) for i in range(2)] for o in range(2)]
    cross = [[both(low_gate, (2 * o, 2 * i + 1), (2 * o + 1, 2 * i)) for i in range(2)] for o in range(2)]
    helds, stage = [], []
    stride = 4 * radix
    for high in range(radix):
        held = []
        for i in range(2):
            held.append(tuple(x[pl.ds(high * 4 + i * 2 + c, rows_hi, stride=stride), :] for c in range(2)))
        helds.append((held, [tuple(roll(v, half) for v in pair) for pair in held]))
        stage.append([])

    def advance(o):
        for high in range(radix):
            held, turned = helds[high]
            total = None
            for i in range(2):
                total = add(total, complex_mul(same[o][i], held[i]))
                total = add(total, complex_mul(cross[o][i], turned[i]))
            stage[high].append(total)

    advance(0)
    sign = jnp.where(field % 2 == 0, -1.0, 1.0)
    mixers = [[entry(split_gate, take, f) for f in range(radix)] for take in range(radix)]
    mixers = [[(re, im * sign) for re, im in line] for line in mixers]

    def merged(out_high, which):
        coefs = [entry(high_gate, out_high, high) for high in range(radix)]
        held = []
        for o in which:
            total = None
            for high in range(radix):
                total = add(total, complex_mul(coefs[high], stage[high][o]))
            held.append(total)
        return held

    def transposed(held):
        turned = {}
        for o in range(2):
            for c in range(2):
                for d in range(2 * o - 3, 2 * o + 2):
                    turned[o, c, d] = roll(held[o][c], d * group)
        blocks = []
        for f in range(radix):
            pair = []
            for flip in range(2):
                block = None
                for o in range(2):
                    for c in range(2):
                        piece = turned[o, c ^ flip, 2 * o + c - f]
                        block = piece if block is None else jnp.where(field == 2 * o + c, piece, block)
                pair.append(block)
            blocks.append(pair)
        return blocks

    def put_main(out_high, held, take):
        real, imag = held[take // 2]
        if take % 2:
            main = jnp.where(first, roll(real, half), imag)
        else:
            main = jnp.where(first, real, roll(imag, half))
        send[out_high * radix + take, :rows_hi] = main

    def put_extra(out_high, blocks, take):
        block = None
        for f in range(radix):
            re, im = mixers[take][f]
            term = re * blocks[f][0] + im * blocks[f][1]
            block = term if block is None else block + term
        own = (take % 2) * 2 + take // 2
        moved = [roll(block[rows_hi - tail :], 2 * group * (own - k)) for k in range(radix) if k != own]
        send[out_high * radix + take, rows_hi:] = jnp.where(
            outer[: rows_hi - tail] == own, jnp.concatenate(moved, axis=0), block[: rows_hi - tail]
        )

    def post(seat, level, rows):
        pltpu.make_async_remote_copy(
            src_ref=send.at[seat * radix + level, rows],
            dst_ref=recv.at[me, rows],
            send_sem=send_sem,
            recv_sem=recv_sem.at[n],
            device_id={"wide": seat, "narrow": level},
            device_id_type=MESH,
        ).start()

    def lowest(first_seat, rows):
        last_seat = first_seat + 1
        alone = (n == 0) & (lax.div(w, 2) == first_seat // 2)
        other_seat = first_seat + last_seat - w

        def body(seat, carry):
            post(seat, 0, rows)
            return carry

        lax.fori_loop(
            jnp.where(alone, other_seat, first_seat), jnp.where(alone, other_seat, last_seat) + 1, body, 0
        )

    whole = pl.ds(0, rows_all)

    def below(level, carry):
        for seat in rows_first:
            post(seat, level, whole)
        return carry

    def above(level, carry):
        for side, pair in ((0, (1, 0)), (1, (3, 2))):
            pl.semaphore_wait(known.at[level, side], 2)
            for seat in pair:
                post(seat, level, whole)
        return carry

    early, opened = {}, {}
    for out_high in range(2):
        early[out_high] = merged(out_high, (0,))
        put_main(out_high, early[out_high], 0)

    def meet():
        @pl.when(core == 0)
        def _():
            pl.semaphore_wait(known.at[n, row], 1)

        @pl.when(row == 0)
        def _():
            pl.semaphore_wait(known.at[n, 1], 2)


    @pl.when(n == 0)
    def _():
        meet()

    lowest(0, pl.ds(0, rows_hi))
    advance(1)
    for out_high in range(2):
        early[out_high] += merged(out_high, (1,))
        opened[out_high] = transposed(early[out_high])
        put_extra(out_high, opened[out_high], 0)

    lowest(0, pl.ds(rows_hi, rows_all - rows_hi))

    for out_high in (2, 3, 0, 1):
        if out_high in early:
            held, blocks = early[out_high], opened[out_high]
        else:
            held = merged(out_high, (0, 1))
            blocks = transposed(held)
        for take in range(1 if out_high in early else 0, radix):
            put_main(out_high, held, take)
            put_extra(out_high, blocks, take)

    def own_level():
        meet()
        for seat in seats[:-1]:
            post(seat, n, whole)

    lowest(2, whole)

    @pl.when(n == 2)
    def _():
        own_level()
        above(3, 0)

    lax.fori_loop(1, n, below, 0)

    @pl.when((n == 1) | (n == 3))
    def _():
        own_level()

    lax.fori_loop(jnp.where(n == 2, radix, n + 1), radix, above, 0)
    recv[me] = send[w * radix + n]

    for begin in range(slots, total_pairs, slots):
        gate.update(merge(order[begin : begin + slots]))
    low = kron_all([gate[pair] for pair in range(start - 2, -1, -1)])
    block = jnp.concatenate(
        [jnp.concatenate([low[0], low[1]], axis=1), jnp.concatenate([-low[1], low[0]], axis=1)], axis=0
    )
    block = jnp.concatenate([jnp.concatenate([block] * radix, axis=0)] * radix, axis=1)
    down = lax.broadcasted_iota(jnp.int32, (LANES, LANES), 0)
    across = lax.broadcasted_iota(jnp.int32, (LANES, LANES), 1)
    grouped = jnp.where(down // (2 * group) == across // (2 * group), block, 0.0).T
    parts = kron_all([gate[pair] for pair in range(start - 1, -1, -1)])
    plain = jnp.concatenate(
        [jnp.concatenate([parts[0], parts[1]], axis=1), jnp.concatenate([-parts[1], parts[0]], axis=1)],
        axis=0,
    ).T
    stripes = range(0, LANES, 2 * group)
    grouped = jnp.concatenate(
        [grouped[at + shift : at + shift + group] for shift in (0, group) for at in stripes], axis=0
    )
    for index, item in enumerate((plain, grouped)):
        lane_hi[index], lane_lo[index] = split(item)
    row_members = [gate[pair] for pair in range(total_pairs - 1, start + 1, -1)]
    real, imag = (split(item) for item in kron_all(row_members))
    for at, into in enumerate((row_hi, row_lo)):
        for source in range(count):
            seat, level = source // radix, source % radix
            rows = slice(source * rows_hi, (source + 1) * rows_hi)
            place = slice(seat * rows_hi, (seat + 1) * rows_hi)
            into[0, level, place] = jnp.concatenate([real[at][rows], imag[at][rows]], axis=1)
            into[1, level, place] = jnp.concatenate([-imag[at][rows], real[at][rows]], axis=1)

    def settled(group, size):
        return pltpu.make_async_remote_copy(
            src_ref=send.at[pl.ds(0, size)],
            dst_ref=recv.at[pl.ds(0, size)],
            send_sem=send_sem,
            recv_sem=recv_sem.at[group],
            device_id={"wide": w, "narrow": n},
            device_id_type=MESH,
        )

    near, far = pairs_of(n)
    settled(near[0], radix - 1).wait_recv()
    settled(near[1], radix).wait_recv()
    acc[...] = contribution(radix, recv, (lane_hi, lane_lo), (row_hi, row_lo), near, n)
    settled(0, count - 1).wait_send()
    for level in far:
        settled(level, radix).wait_recv()


def finish_kernel(radix, recv, acc, lane_hi, lane_lo, row_hi, row_lo, out_hbm, marg_hbm, fin, prob, marg, sems):
    half = LANES // 2
    group = half // radix
    size = acc.shape[1] // 2
    blocks = size // LANES
    n = lax.axis_index("narrow")
    own = (n % 2) * 2 + n // 2
    total = acc[...] + contribution(radix, recv, (lane_hi, lane_lo), (row_hi, row_lo), pairs_of(n)[1], n)
    real, imag = total[:, :size], total[:, size:]
    for block in range(blocks):
        columns = slice(block * LANES, (block + 1) * LANES)
        fin[pl.ds(block * 2, half, stride=2 * blocks), :] = real[:half, columns]
        fin[pl.ds(block * 2 + 1, half, stride=2 * blocks), :] = imag[:half, columns]
    out_copy = pltpu.make_async_copy(fin, out_hbm, sems.at[0])
    out_copy.start()
    density = real * real + imag * imag
    for index in range(radix):
        prob[index] = density[index * group : (index + 1) * group]
    total = prob[n]
    for index in range(radix):
        at = half + group * index
        total = total + jnp.where(own == index, 0.0, density[at : at + group])
    for block in range(blocks):
        marg[pl.ds(block, group, stride=blocks), :] = total[:, block * LANES : (block + 1) * LANES]
    marg_copy = pltpu.make_async_copy(marg, marg_hbm, sems.at[1])
    marg_copy.start()
    out_copy.wait()
    marg_copy.wait()


def window_plan(wide_count, narrow_count, amplitudes, gates_shape):
    layers, pairs, radix = gates_shape[0], gates_shape[1], gates_shape[-1]
    high_bits = (wide_count * narrow_count).bit_length() - 1
    local_bits = amplitudes.bit_length() - 1
    total_bits = high_bits + local_bits
    if high_bits % 2 or local_bits % 2 or wide_count != radix or narrow_count != radix:
        return None
    if 2 * pairs != local_bits:
        return None
    offset = ((layers - 1) * high_bits) % total_bits
    start = offset // 2 - high_bits // 2
    if layers & (layers - 1) or LANES % (layers * radix) or start < 2 or LANES < 3 * layers * radix or offset // 2 >= pairs or 2 * radix**start != LANES:
        return None
    rows_hi = radix ** (pairs - offset // 2)
    if rows_hi % 8:
        return None
    for which in range(total_bits // 2):
        if all((which - layer * (high_bits // 2)) % (total_bits // 2) >= pairs for layer in range(layers)):
            return None
    return (layers, pairs, high_bits // 2, total_bits // 2, start, radix), rows_hi


def merged_local(plan, rows_hi, state, gates):
    radix = plan[-1]
    amplitudes = state.shape[-1]
    rows = amplitudes // LANES
    count = radix * radix
    own = amplitudes // radix // LANES
    x = jnp.swapaxes(state.reshape(2, rows, LANES), 0, 1).reshape(2 * rows, LANES)
    g = jnp.transpose(gates, (1, 2, 3, 4, 0)).reshape(-1, radix, gates.shape[0])
    f32, bf16 = jnp.float32, jnp.bfloat16
    size = count * rows_hi
    message = 2 * rows_hi - rows_hi // radix
    shared = (
        pltpu.VMEM((count, message, LANES), f32),
        pltpu.VMEM((LANES, 2 * size), f32),
        pltpu.VMEM((2, LANES, LANES), bf16),
        pltpu.VMEM((2, LANES, LANES), bf16),
        pltpu.VMEM((2, radix, size // radix, 2 * size), bf16),
        pltpu.VMEM((2, radix, size // radix, 2 * size), bf16),
    )
    held = pl.pallas_call(
        functools.partial(exchange_kernel, plan),
        out_shape=shared,
        in_specs=[pl.BlockSpec(memory_space=pltpu.HBM)] * 2,
        out_specs=[pl.BlockSpec(memory_space=pltpu.VMEM)] * len(shared),
        scratch_shapes=[
            pltpu.VMEM(x.shape, f32),
            pltpu.VMEM(g.shape, f32),
            pltpu.VMEM((count, message, LANES), f32),
            pltpu.SemaphoreType.DMA((2,)),
            pltpu.SemaphoreType.DMA,
            pltpu.SemaphoreType.DMA((radix,)),
            pltpu.SemaphoreType.REGULAR((radix, 2)),
        ],
        compiler_params=pltpu.CompilerParams(
            collective_id=0, has_side_effects=True, vmem_limit_bytes=8 * 2**20
        ),
        name="exchange",
    )(
        pltpu.with_memory_space_constraint(x, pltpu.HBM),
        pltpu.with_memory_space_constraint(g, pltpu.HBM),
    )
    out, marg = pl.pallas_call(
        functools.partial(finish_kernel, radix),
        out_shape=(pltpu.HBM((2 * rows, LANES), f32), pltpu.HBM((own, LANES), f32)),
        in_specs=[pl.BlockSpec(memory_space=pltpu.VMEM)] * len(shared),
        out_specs=[pl.BlockSpec(memory_space=pltpu.HBM)] * 2,
        scratch_shapes=[
            pltpu.VMEM((2 * rows, LANES), f32),
            pltpu.VMEM((radix, LANES // 2 // radix, size), f32),
            pltpu.VMEM((own, LANES), f32),
            pltpu.SemaphoreType.DMA((2,)),
        ],
        compiler_params=pltpu.CompilerParams(vmem_limit_bytes=8 * 2**20),
        name="finish",
    )(*held)
    final = jnp.swapaxes(out.reshape(rows, 2, LANES), 0, 1).reshape(1, 1, 2, amplitudes)
    return final, marg.reshape(1, -1)


def local(state, gates):
    wide_count = lax.axis_size("wide")
    narrow_count = lax.axis_size("narrow")
    amplitudes = state.shape[-1]
    found = window_plan(wide_count, narrow_count, amplitudes, gates.shape)
    if found is not None:
        return merged_local(*found, state, gates)
    flat = state.reshape(2, amplitudes)
    for layer_index in range(gates.shape[0]):
        if layer_index > 0:
            flat = rotate(flat, wide_count, narrow_count)
        flat = apply_layer(flat, gates[layer_index])
    prob = flat[0] * flat[0] + flat[1] * flat[1]
    marginal = lax.psum_scatter(prob, "narrow", scatter_dimension=0, tiled=True)
    return (flat.reshape(1, 1, 2, amplitudes), marginal.reshape(1, -1))


def solution(mesh):
    in_specs = (P(("slices", "wide"), "narrow", None, None), P())
    out_specs = (P(("slices", "wide"), "narrow", None, None), P(("slices", "wide"), "narrow"))
    return jax.shard_map(local, mesh=mesh, in_specs=in_specs, out_specs=out_specs, check_vma=False)
```

```python
import functools

import jax
import jax.numpy as jnp
from jax import lax
from jax.experimental import pallas as pl
from jax.experimental.pallas import tpu as pltpu
from jax.sharding import PartitionSpec as P


def kron_chain(members):
    real_part = members[0][0]
    imag_part = members[0][1]
    for member in members[1:]:
        other_real = member[0]
        other_imag = member[1]
        new_real = jnp.kron(real_part, other_real) - jnp.kron(imag_part, other_imag)
        new_imag = jnp.kron(real_part, other_imag) + jnp.kron(imag_part, other_real)
        real_part, imag_part = (new_real, new_imag)
    return (real_part, imag_part)


def rotate(flat, wide_count, narrow_count):
    devices = wide_count * narrow_count
    amplitudes = flat.shape[1]
    rest = amplitudes // devices
    blocks = flat.reshape(2, rest, devices)
    turned = jnp.swapaxes(blocks, 1, 2)
    moved = lax.all_to_all(turned, ("wide", "narrow"), split_axis=1, concat_axis=1, tiled=True)
    return moved.reshape(2, amplitudes)


def apply_layer(flat, layer_gates):
    amplitudes = flat.shape[1]
    pairs = layer_gates.shape[0]
    upper = amplitudes // 256
    low_real, low_imag = kron_chain([layer_gates[index] for index in range(3, -1, -1)])
    high_real, high_imag = kron_chain([layer_gates[index] for index in range(pairs - 1, 3, -1)])
    blocks = flat.reshape(2, upper, 256)
    real_rows = blocks[0]
    imag_rows = blocks[1]
    highest = lax.Precision.HIGHEST
    next_real = jnp.dot(real_rows, low_real.T, precision=highest) - jnp.dot(
        imag_rows, low_imag.T, precision=highest
    )
    next_imag = jnp.dot(real_rows, low_imag.T, precision=highest) + jnp.dot(
        imag_rows, low_real.T, precision=highest
    )
    final_real = jnp.dot(high_real, next_real, precision=highest) - jnp.dot(
        high_imag, next_imag, precision=highest
    )
    final_imag = jnp.dot(high_imag, next_real, precision=highest) + jnp.dot(
        high_real, next_imag, precision=highest
    )
    return jnp.stack([final_real, final_imag]).reshape(2, amplitudes)


MESH = pl.DeviceIdType.MESH
LANES = 128


def complex_mul(left, right):
    return (
        left[0] * right[0] - left[1] * right[1],
        left[0] * right[1] + left[1] * right[0],
    )


def take_lanes(value, source):
    return jnp.take_along_axis(value, source, axis=1, mode="promise_in_bounds")


def gate_tools(g, plan):
    layers, pairs, shift, total_pairs, _, radix = plan
    shape = (2 * radix, LANES)
    lane = lax.broadcasted_iota(jnp.int32, shape, 1)
    down = lax.broadcasted_iota(jnp.int32, shape, 0)
    width = radix * layers
    layer, row, slot = lane % layers, (lane // layers) % radix, lane // width
    pad = jnp.zeros((radix, LANES - layers), jnp.float32)
    tiles, planes = [], []
    for pair in range(pairs):
        tiles.append([])
        plane = None
        for at in range(radix):
            tile = jnp.concatenate(
                [jnp.concatenate([g[(pair * 2 + c) * radix + at], pad], axis=1) for c in range(2)], axis=0
            )
            tiles[-1].append(tile)
            tile = take_lanes(tile, layer)
            plane = tile if plane is None else jnp.where(row == at, tile, plane)
        planes.append(plane)
    sign = jnp.where(down < radix, -1.0, 1.0)

    def merge(held, direct=False):
        place = held[0] - shift * layer
        for index, pair in enumerate(held[1:]):
            place = jnp.where(slot == index + 1, pair - shift * layer, place)
        for _ in range(-(-layers * shift // total_pairs)):
            place = jnp.where(place < 0, place + total_pairs, place)
        total = jnp.where(down == row, 1.0, 0.0)
        for pair in range(pairs):
            total = jnp.where(place == pair, planes[pair], total)
        step = 1
        while step < layers:
            before = jnp.maximum(layer - step, 0)
            straight, crossed = None, None
            for at in range(radix):
                if direct and step == 1:
                    early = jnp.where(down == at, 1.0, 0.0)
                    previous = jnp.where(place + shift < total_pairs, place + shift, place + shift - total_pairs)
                    for pair in range(pairs):
                        early = jnp.where(previous == pair, take_lanes(tiles[pair][at], before), early)
                else:
                    early = take_lanes(total, slot * width + at * layers + before)
                one_part = total[at : at + 1] * early
                two_part = total[radix + at : radix + at + 1] * early
                straight = one_part if straight is None else straight + one_part
                crossed = two_part if crossed is None else crossed + two_part
            total = straight + sign * pltpu.roll(crossed, radix, 0)
            step *= 2
        return {
            pair: [
                take_lanes(total, jnp.full(shape, index * width + (at + 1) * layers - 1, jnp.int32))
                for at in range(radix)
            ]
            for index, pair in enumerate(held)
        }

    return merge


def kron_all(members):
    radix = len(members[0])
    size = radix ** len(members)
    width = max(size, LANES)
    lane = lax.broadcasted_iota(jnp.int32, (2 * radix, width), 1)
    rows = None
    for place, member in enumerate(reversed(members)):
        field = (lane // radix**place) % radix
        columns = [jnp.concatenate([column] * (width // LANES), axis=1) for column in member]
        spread = columns[-1]
        for index in range(radix - 1):
            spread = jnp.where(field == index, columns[index], spread)
        wide = spread[:radix], spread[radix:]
        if rows is None:
            rows = wide
            continue
        pieces = [
            complex_mul(tuple(part[index : index + 1, :] for part in wide), rows)
            for index in range(radix)
        ]
        rows = tuple(jnp.concatenate([piece[c] for piece in pieces], axis=0) for c in range(2))
    return tuple(part[:, :size] for part in rows)


def split(value):
    high = value.astype(jnp.bfloat16)
    return high, (value - high.astype(jnp.float32)).astype(jnp.bfloat16)


def precise(left, right, contract):
    def one(a, b):
        return lax.dot_general(a, b, (((1,), (contract,)), ((), ())), preferred_element_type=jnp.float32)

    return one(left[0], right[0]) + (one(left[0], right[1]) + one(left[1], right[0]))


def precise_one(a, b):
    return lax.dot_general(a, b, (((1,), (0,)), ((), ())), preferred_element_type=jnp.float32)


def pairs_of(n):
    near = n, jnp.where(n == 0, 1, n - 1)
    return near, (jnp.where(n < 2, 2, 0), jnp.where(n < 3, 3, 1))


def contribution(radix, recv, lanes, rows, levels, n):
    held = jnp.concatenate([recv[pl.ds(level * radix, radix)] for level in levels], axis=0)
    rows_hi = held.shape[1] * radix // (2 * radix - 1)
    tail = rows_hi // radix
    size = held.shape[0] * rows_hi
    wide = LANES // radix
    packed = held[:, rows_hi:]
    outer = lax.broadcasted_iota(jnp.int32, (1, tail, LANES), 2) // wide
    own = (n % 2) * 2 + n // 2
    last = packed[:, :tail]
    for index in range(radix - 1):
        kept = index + jnp.where(own <= index, 1, 0)
        piece = packed[:, index * tail : (index + 1) * tail]
        piece = pltpu.roll(piece, lax.rem(wide * (kept - own) + LANES, LANES), 2)
        last = jnp.where(outer == kept, piece, last)
    turned = []
    for which, value in enumerate((held[:, :rows_hi], jnp.concatenate([packed, last], axis=1))):
        item = precise(tuple(part[which] for part in lanes), split(value.reshape(size, LANES)), 1)
        turned.append(jnp.concatenate([item[: LANES // 2], item[LANES // 2 :]], axis=1))
    matrix = [
        jnp.concatenate([part[c, level] for c in range(2) for level in levels], axis=0) for part in rows
    ]
    high, low = split(jnp.concatenate(turned, axis=0))
    both = precise_one(jnp.concatenate([high, low], axis=0), matrix[0])
    rows = high.shape[0]
    return both[:rows] + (both[rows:] + precise_one(high, matrix[1]))


def greet(semaphore, seat, level):
    pl.semaphore_signal(semaphore, inc=1, device_id={"wide": seat, "narrow": level}, device_id_type=MESH)


def exchange_kernel(plan, x_hbm, g_hbm, recv, acc, lane_hi, lane_lo, row_hi, row_lo, x, g, send,
                    local_sem, send_sem, recv_sem, known):
    layers, pairs, shift, total_pairs, start, radix = plan
    w = lax.axis_index("wide")
    n = lax.axis_index("narrow")
    me = n * radix + w
    count = radix * radix

    barrier = pltpu.get_barrier_semaphore()
    copy_g = pltpu.make_async_copy(g_hbm, g, local_sem.at[0])
    copy_x = pltpu.make_async_copy(x_hbm, x, local_sem.at[1])
    copy_g.start()
    copy_x.start()
    row, core = lax.div(w, 2), lax.rem(w, 2)
    other = 2 * (1 - row)
    ordered = [other + 1, other, 2 * row + 1, 2 * row]
    seats = [other + core, other + 1 - core, 2 * row + 1 - core, w]
    for seat in range(1, radix):
        @pl.when(seat > w)
        def _():
            greet(barrier, seat, n)

    for level in range(1, radix):
        @pl.when(level > n)
        def _():
            for seat in range(radix):
                greet(barrier, seat, level)

    @pl.when(me > 0)
    def _():
        pl.semaphore_wait(barrier, me)

    for level in range(radix - 2, -1, -1):
        @pl.when(level < n)
        def _():
            for seat in range(radix):
                greet(known.at[n, row], seat, level)

    for seat in range(radix - 1):
        @pl.when(seat < w)
        def _():
            greet(known.at[n, row], seat, n)

    copy_g.wait()
    copy_x.wait()

    merge = gate_tools(g, plan)
    order = list(range(start - 1, start + 2)) + list(range(start - 1)) + list(range(start + 2, total_pairs))
    slots = LANES // (radix * layers)
    gate = merge(order[:slots], True)
    split_gate, low_gate, high_gate = (gate[pair] for pair in range(start - 1, start + 2))

    half = LANES // 2
    group = half // radix
    rows_all = send.shape[1]
    rows_hi = rows_all * radix // (2 * radix - 1)
    tail = rows_hi // radix
    shape = (rows_hi, LANES)
    lane = lax.broadcasted_iota(jnp.int32, shape, 1)
    first = lane < half
    field = (lane // group) % radix
    outer = lane // (2 * group)

    def entry(gate, row, column):
        return tuple(
            jnp.broadcast_to(gate[row][at : at + 1], shape) for at in (column, column + radix)
        )

    def both(gate, one, other):
        return tuple(jnp.where(first, a, b) for a, b in zip(entry(gate, *one), entry(gate, *other)))

    def add(total, term):
        return term if total is None else (total[0] + term[0], total[1] + term[1])

    def roll(value, amount):
        amount %= LANES
        return pltpu.roll(value, amount, 1) if amount else value

    same = [[both(low_gate, (2 * o, 2 * i), (2 * o + 1, 2 * i + 1)) for i in range(2)] for o in range(2)]
    cross = [[both(low_gate, (2 * o, 2 * i + 1), (2 * o + 1, 2 * i)) for i in range(2)] for o in range(2)]
    helds, stage = [], []
    stride = 4 * radix
    for high in range(radix):
        held = []
        for i in range(2):
            held.append(tuple(x[pl.ds(high * 4 + i * 2 + c, rows_hi, stride=stride), :] for c in range(2)))
        helds.append((held, [tuple(roll(v, half) for v in pair) for pair in held]))
        stage.append([])

    def advance(o):
        for high in range(radix):
            held, turned = helds[high]
            total = None
            for i in range(2):
                total = add(total, complex_mul(same[o][i], held[i]))
                total = add(total, complex_mul(cross[o][i], turned[i]))
            stage[high].append(total)

    advance(0)
    sign = jnp.where(field % 2 == 0, -1.0, 1.0)
    mixers = [[entry(split_gate, take, f) for f in range(radix)] for take in range(radix)]
    mixers = [[(re, im * sign) for re, im in line] for line in mixers]

    def merged(out_high, which):
        coefs = [entry(high_gate, out_high, high) for high in range(radix)]
        held = []
        for o in which:
            total = None
            for high in range(radix):
                total = add(total, complex_mul(coefs[high], stage[high][o]))
            held.append(total)
        return held

    def transposed(held):
        turned = {}
        for o in range(2):
            for c in range(2):
                for d in range(2 * o - 3, 2 * o + 2):
                    turned[o, c, d] = roll(held[o][c], d * group)
        blocks = []
        for f in range(radix):
            pair = []
            for flip in range(2):
                block = None
                for o in range(2):
                    for c in range(2):
                        piece = turned[o, c ^ flip, 2 * o + c - f]
                        block = piece if block is None else jnp.where(field == 2 * o + c, piece, block)
                pair.append(block)
            blocks.append(pair)
        return blocks

    def put_main(out_high, held, take):
        real, imag = held[take // 2]
        if take % 2:
            main = jnp.where(first, roll(real, half), imag)
        else:
            main = jnp.where(first, real, roll(imag, half))
        send[out_high * radix + take, :rows_hi] = main

    def put_extra(out_high, blocks, take):
        block = None
        for f in range(radix):
            re, im = mixers[take][f]
            term = re * blocks[f][0] + im * blocks[f][1]
            block = term if block is None else block + term
        own = (take % 2) * 2 + take // 2
        moved = [roll(block[rows_hi - tail :], 2 * group * (own - k)) for k in range(radix) if k != own]
        send[out_high * radix + take, rows_hi:] = jnp.where(
            outer[: rows_hi - tail] == own, jnp.concatenate(moved, axis=0), block[: rows_hi - tail]
        )

    def post(seat, level, rows):
        pltpu.make_async_remote_copy(
            src_ref=send.at[seat * radix + level, rows],
            dst_ref=recv.at[me, rows],
            send_sem=send_sem,
            recv_sem=recv_sem.at[n],
            device_id={"wide": seat, "narrow": level},
            device_id_type=MESH,
        ).start()

    def lowest(first_seat, rows):
        last_seat = first_seat + 1
        alone = (n == 0) & (lax.div(w, 2) == first_seat // 2)
        other_seat = first_seat + last_seat - w

        def body(seat, carry):
            post(seat, 0, rows)
            return carry

        lax.fori_loop(
            jnp.where(alone, other_seat, first_seat), jnp.where(alone, other_seat, last_seat) + 1, body, 0
        )

    whole = pl.ds(0, rows_all)

    def below(level, carry):
        for seat in seats:
            post(seat, level, whole)
        return carry

    def above(level, carry):
        for side, pair in ((row, ordered[2:]), (1 - row, ordered[:2])):
            pl.semaphore_wait(known.at[level, side], 2)
            for seat in pair:
                post(seat, level, whole)
        return carry

    early, opened = {}, {}
    for out_high in range(2):
        early[out_high] = merged(out_high, (0,))
        put_main(out_high, early[out_high], 0)

    def meet():
        @pl.when(core == 0)
        def _():
            pl.semaphore_wait(known.at[n, row], 1)

        @pl.when(row == 0)
        def _():
            pl.semaphore_wait(known.at[n, 1], 2)


    @pl.when(n == 0)
    def _():
        meet()

    lowest(0, pl.ds(0, rows_hi))
    advance(1)
    for out_high in range(2):
        early[out_high] += merged(out_high, (1,))
        opened[out_high] = transposed(early[out_high])
        put_extra(out_high, opened[out_high], 0)

    lowest(0, pl.ds(rows_hi, rows_all - rows_hi))

    for out_high in (2, 3, 0, 1):
        if out_high in early:
            held, blocks = early[out_high], opened[out_high]
        else:
            held = merged(out_high, (0, 1))
            blocks = transposed(held)
        for take in range(1 if out_high in early else 0, radix):
            put_main(out_high, held, take)
            put_extra(out_high, blocks, take)

    def own_level():
        meet()
        for seat in seats[:-1]:
            post(seat, n, whole)

    lowest(2, whole)

    @pl.when(n == 2)
    def _():
        above(3, 0)
        own_level()

    lax.fori_loop(1, n, below, 0)

    @pl.when((n == 1) | (n == 3))
    def _():
        own_level()

    lax.fori_loop(jnp.where(n == 2, radix, n + 1), radix, above, 0)
    recv[me] = send[w * radix + n]

    for begin in range(slots, total_pairs, slots):
        gate.update(merge(order[begin : begin + slots]))
    low = kron_all([gate[pair] for pair in range(start - 2, -1, -1)])
    block = jnp.concatenate(
        [jnp.concatenate([low[0], low[1]], axis=1), jnp.concatenate([-low[1], low[0]], axis=1)], axis=0
    )
    block = jnp.concatenate([jnp.concatenate([block] * radix, axis=0)] * radix, axis=1)
    down = lax.broadcasted_iota(jnp.int32, (LANES, LANES), 0)
    across = lax.broadcasted_iota(jnp.int32, (LANES, LANES), 1)
    grouped = jnp.where(down // (2 * group) == across // (2 * group), block, 0.0).T
    parts = kron_all([gate[pair] for pair in range(start - 1, -1, -1)])
    plain = jnp.concatenate(
        [jnp.concatenate([parts[0], parts[1]], axis=1), jnp.concatenate([-parts[1], parts[0]], axis=1)],
        axis=0,
    ).T
    stripes = range(0, LANES, 2 * group)
    grouped = jnp.concatenate(
        [grouped[at + shift : at + shift + group] for shift in (0, group) for at in stripes], axis=0
    )
    for index, item in enumerate((plain, grouped)):
        lane_hi[index], lane_lo[index] = split(item)
    row_members = [gate[pair] for pair in range(total_pairs - 1, start + 1, -1)]
    real, imag = (split(item) for item in kron_all(row_members))
    for at, into in enumerate((row_hi, row_lo)):
        for source in range(count):
            seat, level = source // radix, source % radix
            rows = slice(source * rows_hi, (source + 1) * rows_hi)
            place = slice(seat * rows_hi, (seat + 1) * rows_hi)
            into[0, level, place] = jnp.concatenate([real[at][rows], imag[at][rows]], axis=1)
            into[1, level, place] = jnp.concatenate([-imag[at][rows], real[at][rows]], axis=1)

    def settled(group, size):
        return pltpu.make_async_remote_copy(
            src_ref=send.at[pl.ds(0, size)],
            dst_ref=recv.at[pl.ds(0, size)],
            send_sem=send_sem,
            recv_sem=recv_sem.at[group],
            device_id={"wide": w, "narrow": n},
            device_id_type=MESH,
        )

    near, far = pairs_of(n)
    settled(near[0], radix - 1).wait_recv()
    settled(near[1], radix).wait_recv()
    acc[...] = contribution(radix, recv, (lane_hi, lane_lo), (row_hi, row_lo), near, n)
    settled(0, count - 1).wait_send()
    for level in far:
        settled(level, radix).wait_recv()


def finish_kernel(radix, recv, acc, lane_hi, lane_lo, row_hi, row_lo, out_hbm, marg_hbm, fin, prob, marg, sems):
    half = LANES // 2
    group = half // radix
    size = acc.shape[1] // 2
    blocks = size // LANES
    n = lax.axis_index("narrow")
    own = (n % 2) * 2 + n // 2
    total = acc[...] + contribution(radix, recv, (lane_hi, lane_lo), (row_hi, row_lo), pairs_of(n)[1], n)
    real, imag = total[:, :size], total[:, size:]
    for block in range(blocks):
        columns = slice(block * LANES, (block + 1) * LANES)
        fin[pl.ds(block * 2, half, stride=2 * blocks), :] = real[:half, columns]
        fin[pl.ds(block * 2 + 1, half, stride=2 * blocks), :] = imag[:half, columns]
    out_copy = pltpu.make_async_copy(fin, out_hbm, sems.at[0])
    out_copy.start()
    density = real * real + imag * imag
    for index in range(radix):
        prob[index] = density[index * group : (index + 1) * group]
    total = prob[n]
    for index in range(radix):
        at = half + group * index
        total = total + jnp.where(own == index, 0.0, density[at : at + group])
    for block in range(blocks):
        marg[pl.ds(block, group, stride=blocks), :] = total[:, block * LANES : (block + 1) * LANES]
    marg_copy = pltpu.make_async_copy(marg, marg_hbm, sems.at[1])
    marg_copy.start()
    out_copy.wait()
    marg_copy.wait()


def window_plan(wide_count, narrow_count, amplitudes, gates_shape):
    layers, pairs, radix = gates_shape[0], gates_shape[1], gates_shape[-1]
    high_bits = (wide_count * narrow_count).bit_length() - 1
    local_bits = amplitudes.bit_length() - 1
    total_bits = high_bits + local_bits
    if high_bits % 2 or local_bits % 2 or wide_count != radix or narrow_count != radix:
        return None
    if 2 * pairs != local_bits:
        return None
    offset = ((layers - 1) * high_bits) % total_bits
    start = offset // 2 - high_bits // 2
    if layers & (layers - 1) or LANES % (layers * radix) or start < 2 or LANES < 3 * layers * radix or offset // 2 >= pairs or 2 * radix**start != LANES:
        return None
    rows_hi = radix ** (pairs - offset // 2)
    if rows_hi % 8:
        return None
    for which in range(total_bits // 2):
        if all((which - layer * (high_bits // 2)) % (total_bits // 2) >= pairs for layer in range(layers)):
            return None
    return (layers, pairs, high_bits // 2, total_bits // 2, start, radix), rows_hi


def merged_local(plan, rows_hi, state, gates):
    radix = plan[-1]
    amplitudes = state.shape[-1]
    rows = amplitudes // LANES
    count = radix * radix
    own = amplitudes // radix // LANES
    x = jnp.swapaxes(state.reshape(2, rows, LANES), 0, 1).reshape(2 * rows, LANES)
    g = jnp.transpose(gates, (1, 2, 3, 4, 0)).reshape(-1, radix, gates.shape[0])
    f32, bf16 = jnp.float32, jnp.bfloat16
    size = count * rows_hi
    message = 2 * rows_hi - rows_hi // radix
    shared = (
        pltpu.VMEM((count, message, LANES), f32),
        pltpu.VMEM((LANES, 2 * size), f32),
        pltpu.VMEM((2, LANES, LANES), bf16),
        pltpu.VMEM((2, LANES, LANES), bf16),
        pltpu.VMEM((2, radix, size // radix, 2 * size), bf16),
        pltpu.VMEM((2, radix, size // radix, 2 * size), bf16),
    )
    held = pl.pallas_call(
        functools.partial(exchange_kernel, plan),
        out_shape=shared,
        in_specs=[pl.BlockSpec(memory_space=pltpu.HBM)] * 2,
        out_specs=[pl.BlockSpec(memory_space=pltpu.VMEM)] * len(shared),
        scratch_shapes=[
            pltpu.VMEM(x.shape, f32),
            pltpu.VMEM(g.shape, f32),
            pltpu.VMEM((count, message, LANES), f32),
            pltpu.SemaphoreType.DMA((2,)),
            pltpu.SemaphoreType.DMA,
            pltpu.SemaphoreType.DMA((radix,)),
            pltpu.SemaphoreType.REGULAR((radix, 2)),
        ],
        compiler_params=pltpu.CompilerParams(
            collective_id=0, has_side_effects=True, vmem_limit_bytes=8 * 2**20
        ),
        name="exchange",
    )(
        pltpu.with_memory_space_constraint(x, pltpu.HBM),
        pltpu.with_memory_space_constraint(g, pltpu.HBM),
    )
    out, marg = pl.pallas_call(
        functools.partial(finish_kernel, radix),
        out_shape=(pltpu.HBM((2 * rows, LANES), f32), pltpu.HBM((own, LANES), f32)),
        in_specs=[pl.BlockSpec(memory_space=pltpu.VMEM)] * len(shared),
        out_specs=[pl.BlockSpec(memory_space=pltpu.HBM)] * 2,
        scratch_shapes=[
            pltpu.VMEM((2 * rows, LANES), f32),
            pltpu.VMEM((radix, LANES // 2 // radix, size), f32),
            pltpu.VMEM((own, LANES), f32),
            pltpu.SemaphoreType.DMA((2,)),
        ],
        compiler_params=pltpu.CompilerParams(vmem_limit_bytes=8 * 2**20),
        name="finish",
    )(*held)
    final = jnp.swapaxes(out.reshape(rows, 2, LANES), 0, 1).reshape(1, 1, 2, amplitudes)
    return final, marg.reshape(1, -1)


def local(state, gates):
    wide_count = lax.axis_size("wide")
    narrow_count = lax.axis_size("narrow")
    amplitudes = state.shape[-1]
    found = window_plan(wide_count, narrow_count, amplitudes, gates.shape)
    if found is not None:
        return merged_local(*found, state, gates)
    flat = state.reshape(2, amplitudes)
    for layer_index in range(gates.shape[0]):
        if layer_index > 0:
            flat = rotate(flat, wide_count, narrow_count)
        flat = apply_layer(flat, gates[layer_index])
    prob = flat[0] * flat[0] + flat[1] * flat[1]
    marginal = lax.psum_scatter(prob, "narrow", scatter_dimension=0, tiled=True)
    return (flat.reshape(1, 1, 2, amplitudes), marginal.reshape(1, -1))


def solution(mesh):
    in_specs = (P(("slices", "wide"), "narrow", None, None), P())
    out_specs = (P(("slices", "wide"), "narrow", None, None), P(("slices", "wide"), "narrow"))
    return jax.shard_map(local, mesh=mesh, in_specs=in_specs, out_specs=out_specs, check_vma=False)
```
